32 devices in a mesh: dp: 4 (over x, y), sp: 8 (over z, core).
Axes of the slice: x: 2, y: 2, z: 4, core: 2. Of those that a mesh axis runs over, the one named last changes fastest.
Arguments:
- x_in: bfloat16 [128, 512, 1024], P('dp', 'sp'), parts along dimension 0
- dy_out: bfloat16 [128, 512, 1024], P('dp', 'sp'), parts along dimension 0
- w_query: bfloat16 [1024, 1024], replicated
- w_key: bfloat16 [1024, 1024], replicated
- w_value: bfloat16 [1024, 1024], replicated
- w_beta: bfloat16 [1024, 8], replicated
- conv_query: bfloat16 [4, 1024], replicated
- conv_key: bfloat16 [4, 1024], replicated
- conv_value: bfloat16 [4, 1024], replicated
- w_gate: bfloat16 [1024, 1024], replicated
- norm_weight: bfloat16 [128], replicated
- w_out: bfloat16 [1024, 1024], replicated
Outputs:
- output 1: bfloat16 [128, 512, 1024], P('dp', 'sp'), parts along dimension 0
- output 2: bfloat16 [128, 512, 1024], P('dp', 'sp'), parts along dimension 0
- output 3: float32 [4096, 1024], P('dp'), parts along dimension 0
- output 4: float32 [4096, 1024], P('dp'), parts along dimension 0
- output 5: float32 [4096, 1024], P('dp'), parts along dimension 0
- output 6: float32 [4096, 8], P('dp'), parts along dimension 0
- output 7: float32 [16, 1024], P('dp'), parts along dimension 0
- output 8: float32 [16, 1024], P('dp'), parts along dimension 0
- output 9: float32 [16, 1024], P('dp'), parts along dimension 0
- output 10: float32 [4096, 1024], P('dp'), parts along dimension 0
- output 11: float32 [512], P('dp'), parts along dimension 0
- output 12: float32 [4096, 1024], P('dp'), parts along dimension 0
There are 4 independent parts. The reference program is written for one: setup_inputs(seed, part) draws one part's arguments, and reference() takes and returns one part's arrays. A program takes and returns all parts, laid end to end along the dimension named above; an argument that names none is the same for every part.
All inputs are finite; a program needn't handle non-finite values.
Results may differ from the reference program's by a relative error of at most 0.0180959.
Values are sent between devices in bfloat16 or wider.
A program may use at most 1 GiB of HBM per device.

```python
import jax
import jax.numpy as jnp
from jax import lax

BATCH_SIZE = 32
SEQ_LEN = 512
MODEL_DIM = 1024
NUM_HEADS = 8
HEAD_DIM = 128
BLOCK_LEN = 64
CONV_TAPS = 4


def setup_inputs(seed: int = 0, part: int = 0) -> dict:
    part_key = jax.random.fold_in(jax.random.key(seed), part)
    data_keys = jax.random.split(part_key, 2)
    weight_keys = jax.random.split(jax.random.key(seed + 1), 10)
    w_scale = MODEL_DIM ** -0.5
    act_shape = (BATCH_SIZE, SEQ_LEN, MODEL_DIM)
    square = (MODEL_DIM, MODEL_DIM)
    taps_shape = (CONV_TAPS, MODEL_DIM)

    def normal_bf16(rand_key, arr_shape, arr_scale):
        return (jax.random.normal(rand_key, arr_shape, jnp.float32) * arr_scale).astype(jnp.bfloat16)

    norm_draw = 0.3 + jax.random.normal(weight_keys[9], (HEAD_DIM,), jnp.float32)
    return {
        'x_in': normal_bf16(data_keys[0], act_shape, 1.0),
        'dy_out': normal_bf16(data_keys[1], act_shape, 1.0),
        'w_query': normal_bf16(weight_keys[0], square, w_scale),
        'w_key': normal_bf16(weight_keys[1], square, w_scale),
        'w_value': normal_bf16(weight_keys[2], square, w_scale),
        'w_beta': normal_bf16(weight_keys[3], (MODEL_DIM, NUM_HEADS), w_scale),
        'conv_query': normal_bf16(weight_keys[4], taps_shape, 0.5),
        'conv_key': normal_bf16(weight_keys[5], taps_shape, 0.5),
        'conv_value': normal_bf16(weight_keys[6], taps_shape, 0.5),
        'w_gate': normal_bf16(weight_keys[7], square, w_scale),
        'norm_weight': norm_draw.astype(jnp.bfloat16),
        'w_out': normal_bf16(weight_keys[8], square, w_scale),
    }


def conv_silu(proj_in, tap_weights):
    seq_len = proj_in.shape[1]
    padded = jnp.pad(proj_in.astype(jnp.float32), ((0, 0), (CONV_TAPS - 1, 0), (0, 0)))
    conv_sum = padded[:, 0:seq_len] * tap_weights[0]
    for tap_idx in range(1, CONV_TAPS):
        conv_sum = conv_sum + padded[:, tap_idx:tap_idx + seq_len] * tap_weights[tap_idx]
    return jax.nn.silu(conv_sum)


def head_l2(values):
    shaped = values.reshape(values.shape[:-1] + (-1, HEAD_DIM))
    scaled = shaped * lax.rsqrt(jnp.sum(shaped * shaped, axis=-1, keepdims=True) + 1e-6)
    return scaled.reshape(values.shape)


def delta_rule(queries, key_vecs, values, beta_tok):
    n_seqs, seq_len, model_dim = queries.shape
    n_heads = model_dim // HEAD_DIM
    n_blocks = seq_len // BLOCK_LEN

    def to_blocks(array_in):
        return array_in.astype(jnp.float32).reshape(n_seqs, n_blocks, BLOCK_LEN, n_heads, HEAD_DIM).transpose(1, 0, 3, 2, 4)

    q_blk = to_blocks(queries)
    k_blk = to_blocks(key_vecs)
    v_blk = to_blocks(values)
    b_blk = beta_tok.astype(jnp.float32).reshape(n_seqs, n_blocks, BLOCK_LEN, n_heads).transpose(1, 0, 3, 2)
    positions = jnp.arange(BLOCK_LEN)
    strict = (positions[:, None] > positions[None, :]).astype(jnp.float32)
    inclusive = (positions[:, None] >= positions[None, :]).astype(jnp.float32)
    gram_mat = jnp.einsum('nbhca,nbhsa->nbhcs', k_blk, k_blk)
    system = jnp.eye(BLOCK_LEN, dtype=jnp.float32) + b_blk[..., None] * gram_mat * strict
    rhs_mat = jnp.concatenate([k_blk, v_blk], axis=-1) * b_blk[..., None]
    solved = jnp.linalg.solve(system, rhs_mat)
    scores = jnp.einsum('nbhca,nbhsa->nbhcs', q_blk, k_blk) * inclusive

    def scan_step(state_mat, block_in):
        w_n, u_n, q_n, k_n, s_n = block_in
        delta_mat = u_n - jnp.einsum('bhca,bhae->bhce', w_n, state_mat)
        out_n = jnp.einsum('bhca,bhae->bhce', q_n, state_mat) + jnp.einsum('bhcs,bhse->bhce', s_n, delta_mat)
        state_mat = state_mat + jnp.einsum('bhca,bhce->bhae', k_n, delta_mat)
        return state_mat, out_n

    init_state = jnp.zeros((n_seqs, n_heads, HEAD_DIM, HEAD_DIM), jnp.float32)
    block_outs = lax.scan(scan_step, init_state, (solved[..., :HEAD_DIM], solved[..., HEAD_DIM:], q_blk, k_blk, scores))[1]
    return block_outs.transpose(1, 0, 3, 2, 4).reshape(n_seqs, seq_len, model_dim)


def layer_forward(x_f, weights):
    w_query, w_key, w_value, w_beta, conv_query, conv_key, conv_value, w_gate, norm_weight, w_out = weights
    n_seqs, seq_len, model_dim = x_f.shape
    flat_x = x_f.reshape(n_seqs * seq_len, model_dim)

    def project(weight):
        return jnp.dot(flat_x, weight, preferred_element_type=jnp.float32).astype(jnp.bfloat16).reshape(n_seqs, seq_len, -1)

    queries = head_l2(conv_silu(project(w_query), conv_query)).astype(jnp.bfloat16)
    key_vecs = head_l2(conv_silu(project(w_key), conv_key)).astype(jnp.bfloat16)
    values = conv_silu(project(w_value), conv_value).astype(jnp.bfloat16)
    beta_tok = jax.nn.sigmoid(project(w_beta).astype(jnp.float32)).astype(jnp.bfloat16)
    attn_out = delta_rule(queries, key_vecs, values, beta_tok).astype(jnp.bfloat16)
    gate_pre = project(w_gate)
    shaped = attn_out.astype(jnp.float32).reshape(n_seqs, seq_len, -1, HEAD_DIM)
    normed = shaped * lax.rsqrt(jnp.mean(shaped * shaped, axis=-1, keepdims=True) + 1e-5) * norm_weight
    hidden = (normed.reshape(n_seqs, seq_len, model_dim) * jax.nn.silu(gate_pre.astype(jnp.float32))).astype(jnp.bfloat16)
    y_flat = jnp.dot(hidden.reshape(n_seqs * seq_len, model_dim), w_out, preferred_element_type=jnp.float32)
    return y_flat.astype(jnp.bfloat16).reshape(n_seqs, seq_len, model_dim)


def reference(x_in, dy_out, w_query, w_key, w_value, w_beta, conv_query, conv_key, conv_value, w_gate, norm_weight, w_out):
    weights = tuple(array_in.astype(jnp.float32) for array_in in (w_query, w_key, w_value, w_beta, conv_query, conv_key, conv_value, w_gate, norm_weight, w_out))
    y_out, pullback = jax.vjp(layer_forward, x_in.astype(jnp.float32), weights)
    dx_f, grad_list = pullback(dy_out)
    return (y_out, dx_f.astype(jnp.bfloat16), grad_list[0], grad_list[1], grad_list[2], grad_list[3], grad_list[4], grad_list[5], grad_list[6], grad_list[7], grad_list[8], grad_list[9])
```

```python
import functools
import jax
import jax.numpy as jnp
from jax import lax
from jax.experimental import pallas as pl
from jax.experimental.pallas import tpu as pltpu
from jax.sharding import PartitionSpec as P

HEAD_DIM = 128
CONV_TAPS = 4
PAD = CONV_TAPS - 1
SEND_SLOTS = 4
F32 = jnp.float32
BF16 = jnp.bfloat16
MESH = pl.DeviceIdType.MESH
VMEM_LIMIT = 60 * 1024 * 1024


def project(act_in, weight):
    return jnp.einsum('btd,de->bte', act_in, weight, preferred_element_type=F32)


def back_project(grad_in, weight):
    return jnp.einsum('bte,de->btd', grad_in, weight, preferred_element_type=F32)


def weight_grad(act_in, grad_in):
    return jnp.einsum('btd,bte->de', act_in, grad_in, preferred_element_type=F32)


def bdot(lhs, rhs, lhs_dim, rhs_dim):
    return lax.dot_general(lhs, rhs, (((lhs_dim,), (rhs_dim,)), ((0,), (0,))), preferred_element_type=F32)


def split(value):
    high = value.astype(BF16)
    return high, (value - high.astype(F32)).astype(BF16)


def dot_er(lhs, rhs, lhs_dim, rhs_dim):
    return bdot(lhs, rhs[0], lhs_dim, rhs_dim) + bdot(lhs, rhs[1], lhs_dim, rhs_dim)


def dot_re(lhs, rhs, lhs_dim, rhs_dim):
    return bdot(lhs[0], rhs, lhs_dim, rhs_dim) + bdot(lhs[1], rhs, lhs_dim, rhs_dim)


def dot_rr(lhs, rhs, lhs_dim, rhs_dim):
    return bdot(lhs[0], rhs[0], lhs_dim, rhs_dim) + (bdot(lhs[0], rhs[1], lhs_dim, rhs_dim) + bdot(lhs[1], rhs[0], lhs_dim, rhs_dim))


def block_inverse(low_mat, row_idx, col_idx):
    size = low_mat.shape[-1]
    eye = (row_idx == col_idx).astype(F32)
    low_split = split(low_mat)
    inv = eye - jnp.where(row_idx // 2 == col_idx // 2, low_mat, 0.0)
    width = 2
    while width < size:
        fresh = (row_idx // (2 * width) == col_idx // (2 * width)) & (row_idx // width != col_idx // width)
        corner = jnp.where(fresh, low_mat, 0.0).astype(BF16)
        inv_b = inv.astype(BF16)
        inv = inv - bdot(bdot(inv_b, corner, 2, 1).astype(BF16), inv_b, 2, 1)
        width *= 2
    inv_split = split(inv)
    resid = eye - inv - dot_rr(low_split, inv_split, 2, 1)
    return inv + bdot(inv_split[0], resid.astype(BF16), 2, 1)


def head_cols(head):
    return pl.ds(pl.multiple_of(head * HEAD_DIM, HEAD_DIM), HEAD_DIM)


def head_columns(array_in, n_heads):
    return jnp.concatenate([array_in[:, head:head + 1][None] for head in range(n_heads)], axis=0)


def entry_barrier(me, groups):
    barrier = pltpu.get_barrier_semaphore()
    for step in (1, groups - 1):
        pl.semaphore_signal(barrier, inc=1, device_id={'sp': lax.rem(me + step, groups)}, device_id_type=MESH)
    pl.semaphore_wait(barrier, 2)


def conv_rows(ext_ref, branch, cols, taps, seq_dev):
    total = ext_ref[branch, pl.ds(8 - PAD, seq_dev), cols] * taps[0:1]
    for tap_idx in range(1, CONV_TAPS):
        total = total + ext_ref[branch, pl.ds(8 - PAD + tap_idx, seq_dev), cols] * taps[tap_idx:tap_idx + 1]
    return total


def fill_ext(ext_ref, p_refs, tail_ref, cols, head, model_dim):
    seq_dev = p_refs[0].shape[1]
    for branch in range(3):
        tail_cols = pl.ds(pl.multiple_of(branch * model_dim + head * HEAD_DIM, HEAD_DIM), HEAD_DIM)
        ext_ref[branch, pl.ds(8 - PAD, PAD), cols] = tail_ref[0, :, tail_cols].astype(F32)
        ext_ref[branch, pl.ds(8, seq_dev), cols] = p_refs[branch][0, :, cols].astype(F32)


def forward_kernel(groups, pq_ref, pk_ref, pv_ref, tail_ref, taps_ref, logit_ref, z_ref, dh_ref, norm_ref,
                   h_ref, dz_ref, do_ref, q_ref, k_ref, t_ref, s_ref, r_ref, d_ref, dnorm_ref,
                   recv, send, ext, v_buf, o_buf, send_sem, recv_sem):
    step = pl.program_id(0)
    n_steps = pl.num_programs(0)
    me = lax.axis_index('sp')
    seq_dev = pq_ref.shape[1]
    model_dim = pq_ref.shape[2]
    n_heads = model_dim // HEAD_DIM
    slot = lax.rem(step, SEND_SLOTS)

    def hop(slot_idx, step_idx):
        return pltpu.make_async_remote_copy(
            src_ref=send.at[slot_idx], dst_ref=recv.at[step_idx], send_sem=send_sem.at[slot_idx], recv_sem=recv_sem.at[step_idx],
            device_id={'sp': lax.rem(me + 1, groups)}, device_id_type=MESH)

    @pl.when(step == 0)
    def _():
        entry_barrier(me, groups)
        dnorm_ref[...] = jnp.zeros_like(dnorm_ref)

    def act_head(head, carry):
        cols = head_cols(head)
        fill_ext(ext, (pq_ref, pk_ref, pv_ref), tail_ref, cols, head, model_dim)
        for branch in range(3):
            act = jax.nn.silu(conv_rows(ext, branch, cols, taps_ref[branch, :, cols], seq_dev))
            if branch < 2:
                act = act * lax.rsqrt(jnp.sum(act * act, axis=-1, keepdims=True) + 1e-6)
                (q_ref, k_ref)[branch][0, head] = act.astype(BF16)
            else:
                v_buf[head] = act.astype(BF16)
        return carry

    lax.fori_loop(0, n_heads, act_head, 0)

    beta = jax.nn.sigmoid(logit_ref[0].astype(F32)).astype(BF16).astype(F32)
    beta3 = head_columns(beta, n_heads)
    q_all = q_ref[0]
    k_all = k_ref[0]
    row_idx = lax.broadcasted_iota(jnp.int32, (1, seq_dev, seq_dev), 1)
    col_idx = lax.broadcasted_iota(jnp.int32, (1, seq_dev, seq_dev), 2)
    gram = bdot(k_all, k_all, 2, 2)
    t_ref[0] = block_inverse(jnp.where(row_idx > col_idx, beta3 * gram, 0.0), row_idx, col_idx)

    @pl.when(me > 0)
    def _():
        hop(slot, step).wait_recv()

    @pl.when(me == 0)
    def _():
        recv[step] = jnp.zeros(recv.shape[1:], F32)

    @pl.when((me < groups - 1) & (step >= SEND_SLOTS))
    def _():
        hop(slot, step).wait_send()

    state = recv[step]
    s_ref[0] = state
    state_split = split(state)
    resid = v_buf[...].astype(F32) - dot_er(k_all, state_split, 2, 1)
    r_ref[0] = resid
    delta = dot_rr(split(t_ref[0]), split(beta3 * resid), 2, 1)
    d_ref[0] = delta
    delta_split = split(delta)
    send[slot] = state + dot_er(k_all, delta_split, 1, 1)
    scores = jnp.where(row_idx >= col_idx, bdot(q_all, k_all, 2, 2), 0.0)
    o_buf[...] = (dot_er(q_all, state_split, 2, 1) + dot_rr(split(scores), delta_split, 2, 1)).astype(BF16).astype(F32)

    @pl.when(me < groups - 1)
    def _():
        hop(slot, step).start()

    def post_head(head, carry):
        cols = head_cols(head)
        attn = o_buf[head]
        norm_w = norm_ref[...]
        z_in = z_ref[0, :, cols].astype(F32)
        dh_in = dh_ref[0, :, cols].astype(F32)
        inv_rms = lax.rsqrt(jnp.mean(attn * attn, axis=-1, keepdims=True) + 1e-5)
        unit = attn * inv_rms
        normed = unit * norm_w
        sig = jax.nn.sigmoid(z_in)
        gate = z_in * sig
        h_ref[0, :, cols] = (normed * gate).astype(BF16)
        d_normed = dh_in * gate
        dz_ref[0, :, cols] = (dh_in * normed * (sig * (1.0 + z_in * (1.0 - sig)))).astype(BF16)
        d_unit = d_normed * norm_w
        dnorm_ref[...] += jnp.sum((d_normed * unit).reshape(seq_dev // 8, 8, HEAD_DIM), axis=0)
        do_ref[0, head] = (inv_rms * (d_unit - unit * jnp.mean(unit * d_unit, axis=-1, keepdims=True))).astype(BF16)
        return carry

    lax.fori_loop(0, n_heads, post_head, 0)

    @pl.when((me < groups - 1) & (step == n_steps - 1))
    def _():
        for back in range(min(SEND_SLOTS, recv.shape[0])):
            last = recv.shape[0] - 1 - back
            hop(last % SEND_SLOTS, last).wait_send()


def backward_kernel(groups, pq_ref, pk_ref, pv_ref, tail_ref, taps_ref, logit_ref, do_ref, q_ref, k_ref, t_ref, s_ref, r_ref, d_ref,
                    dpq_ref, dpk_ref, dpv_ref, dlogit_ref, dtaps_ref,
                    recv, send, front, front_send, ext, dext, dact, send_sem, recv_sem, fsend_sem, frecv_sem):
    step = pl.program_id(0)
    n_steps = pl.num_programs(0)
    me = lax.axis_index('sp')
    seq_dev = pq_ref.shape[1]
    model_dim = pq_ref.shape[2]
    n_heads = model_dim // HEAD_DIM
    slot = lax.rem(step, SEND_SLOTS)
    to_prev = lax.rem(me + groups - 1, groups)

    def hop(slot_idx, step_idx):
        return pltpu.make_async_remote_copy(
            src_ref=send.at[slot_idx], dst_ref=recv.at[step_idx], send_sem=send_sem.at[slot_idx], recv_sem=recv_sem.at[step_idx],
            device_id={'sp': to_prev}, device_id_type=MESH)

    def front_hop(slot_idx, step_idx):
        return pltpu.make_async_remote_copy(
            src_ref=front_send.at[slot_idx], dst_ref=front.at[step_idx], send_sem=fsend_sem.at[slot_idx], recv_sem=frecv_sem.at[step_idx],
            device_id={'sp': to_prev}, device_id_type=MESH)

    @pl.when(step == 0)
    def _():
        entry_barrier(me, groups)
        dtaps_ref[...] = jnp.zeros_like(dtaps_ref)

    sig_beta = jax.nn.sigmoid(logit_ref[0].astype(F32))
    beta3 = head_columns(sig_beta.astype(BF16).astype(F32), n_heads)
    q_all = q_ref[0]
    k_all = k_ref[0]
    d_out = do_ref[0]
    row_idx = lax.broadcasted_iota(jnp.int32, (1, seq_dev, seq_dev), 1)
    col_idx = lax.broadcasted_iota(jnp.int32, (1, seq_dev, seq_dev), 2)
    gram = bdot(k_all, k_all, 2, 2)
    scores = jnp.where(row_idx >= col_idx, bdot(q_all, k_all, 2, 2), 0.0)
    t_split = split(t_ref[0])
    delta_split = split(d_ref[0])
    state_split = split(s_ref[0])
    d_delta_own = dot_re(split(scores), d_out, 1, 1)
    state_own = bdot(q_all, d_out, 1, 1)
    d_scores = jnp.where(row_idx >= col_idx, dot_er(d_out, delta_split, 2, 2), 0.0).astype(BF16)
    dact[0] = (dot_er(d_out, state_split, 2, 2) + bdot(d_scores, k_all, 2, 1)).astype(BF16)

    @pl.when(me < groups - 1)
    def _():
        hop(slot, step).wait_recv()

    @pl.when(me == groups - 1)
    def _():
        recv[step] = jnp.zeros(recv.shape[1:], F32)
        front[step] = jnp.zeros(front.shape[1:], F32)

    @pl.when((me > 0) & (step >= SEND_SLOTS))
    def _():
        hop(slot, step).wait_send()
        front_hop(slot, step).wait_send()

    d_state = recv[step]
    d_state_split = split(d_state)
    d_delta = d_delta_own + dot_er(k_all, d_state_split, 2, 1)
    d_rhs = dot_rr(t_split, split(d_delta), 1, 1)
    d_resid = beta3 * d_rhs
    d_resid_split = split(d_resid)
    send[slot] = d_state + state_own - dot_er(k_all, d_resid_split, 1, 1)
    dact[2] = d_resid.astype(BF16)
    d_low = jnp.where(row_idx > col_idx, -dot_rr(split(d_rhs), delta_split, 2, 2), 0.0)
    d_beta = jnp.sum(d_rhs * r_ref[0], axis=-1, keepdims=True) + jnp.sum(d_low * gram, axis=-1, keepdims=True)
    d_gram = (beta3 * d_low).astype(BF16)
    d_key = dot_rr(delta_split, d_state_split, 2, 2) - dot_rr(d_resid_split, state_split, 2, 2)
    d_key = d_key + bdot(d_gram, k_all, 2, 1) + bdot(d_gram, k_all, 1, 1) + bdot(d_scores, q_all, 1, 1)
    dact[1] = d_key.astype(BF16)
    lane_idx = lax.broadcasted_iota(jnp.int32, (seq_dev, n_heads), 1)
    beta_grad = jnp.zeros((seq_dev, n_heads), F32)
    for head in range(n_heads):
        beta_grad = beta_grad + jnp.where(lane_idx == head, d_beta[head], 0.0)
    dlogit_ref[0] = (beta_grad.astype(BF16).astype(F32) * sig_beta * (1.0 - sig_beta)).astype(BF16)

    @pl.when(me > 0)
    def _():
        hop(slot, step).start()

    def act_head(head, carry):
        cols = head_cols(head)
        fill_ext(ext, (pq_ref, pk_ref, pv_ref), tail_ref, cols, head, model_dim)
        for branch in range(3):
            conv_sum = conv_rows(ext, branch, cols, taps_ref[branch, :, cols], seq_dev)
            sig = jax.nn.sigmoid(conv_sum)
            d_act = dact[branch, head].astype(F32)
            if branch < 2:
                act = conv_sum * sig
                inv_norm = lax.rsqrt(jnp.sum(act * act, axis=-1, keepdims=True) + 1e-6)
                unit = act * inv_norm
                d_act = inv_norm * (d_act - unit * jnp.sum(unit * d_act, axis=-1, keepdims=True))
            d_conv = d_act * (sig * (1.0 + conv_sum * (1.0 - sig)))
            dext[branch, pl.ds(0, seq_dev), cols] = d_conv
            front_send[slot, branch, :, cols] = d_conv[0:8]
            for tap_idx in range(CONV_TAPS):
                prod = d_conv * ext[branch, pl.ds(8 - PAD + tap_idx, seq_dev), cols]
                dtaps_ref[branch, tap_idx, :, cols] += jnp.sum(prod.reshape(seq_dev // 8, 8, HEAD_DIM), axis=0)
        return carry

    lax.fori_loop(0, n_heads, act_head, 0)

    @pl.when(me > 0)
    def _():
        front_hop(slot, step).start()

    @pl.when(me < groups - 1)
    def _():
        front_hop(slot, step).wait_recv()

    def conv_head(head, carry):
        cols = head_cols(head)
        for branch in range(3):
            taps = taps_ref[branch, :, cols]
            dext[branch, pl.ds(seq_dev, 8), cols] = front[step, branch, :, cols]
            total = dext[branch, pl.ds(PAD, seq_dev), cols] * taps[0:1]
            for tap_idx in range(1, CONV_TAPS):
                total = total + dext[branch, pl.ds(PAD - tap_idx, seq_dev), cols] * taps[tap_idx:tap_idx + 1]
            (dpq_ref, dpk_ref, dpv_ref)[branch][0, :, cols] = total.astype(BF16)
        return carry

    lax.fori_loop(0, n_heads, conv_head, 0)

    @pl.when((me > 0) & (step == n_steps - 1))
    def _():
        for back in range(min(SEND_SLOTS, recv.shape[0])):
            last = recv.shape[0] - 1 - back
            hop(last % SEND_SLOTS, last).wait_send()
            front_hop(last % SEND_SLOTS, last).wait_send()


def seq_block(shape):
    return pl.BlockSpec((1,) + tuple(shape[1:]), lambda step: (step,) + (0,) * (len(shape) - 1))


def whole_block(shape):
    return pl.BlockSpec(tuple(shape), lambda step: (0,) * len(shape))


def run_forward(groups, projs, tails, taps, logits, gate_pre, d_hidden, norm_f):
    n_seqs, seq_dev, model_dim = gate_pre.shape
    n_heads = model_dim // HEAD_DIM
    tok = jax.ShapeDtypeStruct((n_seqs, seq_dev, model_dim), BF16)
    per_head_b = jax.ShapeDtypeStruct((n_seqs, n_heads, seq_dev, HEAD_DIM), BF16)
    per_head_f = jax.ShapeDtypeStruct((n_seqs, n_heads, seq_dev, HEAD_DIM), F32)
    outs = [tok, tok, per_head_b, per_head_b, per_head_b,
            jax.ShapeDtypeStruct((n_seqs, n_heads, seq_dev, seq_dev), F32),
            jax.ShapeDtypeStruct((n_seqs, n_heads, HEAD_DIM, HEAD_DIM), F32),
            per_head_f, per_head_f, jax.ShapeDtypeStruct((8, HEAD_DIM), F32)]
    ins = [*projs, tails, taps, logits, gate_pre, d_hidden, norm_f]
    return pl.pallas_call(
        functools.partial(forward_kernel, groups),
        grid=(n_seqs,),
        out_shape=outs,
        in_specs=[seq_block(arr.shape) for arr in ins[:4]] + [whole_block(taps.shape)] + [seq_block(arr.shape) for arr in ins[5:8]] + [whole_block(norm_f.shape)],
        out_specs=[seq_block(out.shape) for out in outs[:-1]] + [whole_block(outs[-1].shape)],
        scratch_shapes=[
            pltpu.VMEM((n_seqs, n_heads, HEAD_DIM, HEAD_DIM), F32),
            pltpu.VMEM((SEND_SLOTS, n_heads, HEAD_DIM, HEAD_DIM), F32),
            pltpu.VMEM((3, seq_dev + 8, model_dim), F32),
            pltpu.VMEM((n_heads, seq_dev, HEAD_DIM), BF16),
            pltpu.VMEM((n_heads, seq_dev, HEAD_DIM), F32),
            pltpu.SemaphoreType.DMA((SEND_SLOTS,)),
            pltpu.SemaphoreType.DMA((n_seqs,)),
        ],
        compiler_params=pltpu.CompilerParams(collective_id=0, has_side_effects=True, vmem_limit_bytes=VMEM_LIMIT, dimension_semantics=('arbitrary',)),
        cost_estimate=pl.CostEstimate(flops=200_000_000_000, bytes_accessed=120_000_000, transcendentals=0),
        name='delta_forward',
    )(*ins)


def run_backward(groups, projs, tails, taps, logits, d_attn, q_act, k_act, t_mat, s_mat, r_mat, d_mat):
    n_seqs, seq_dev, model_dim = projs[0].shape
    n_heads = model_dim // HEAD_DIM
    tok = jax.ShapeDtypeStruct((n_seqs, seq_dev, model_dim), BF16)
    outs = [tok, tok, tok, jax.ShapeDtypeStruct(logits.shape, BF16), jax.ShapeDtypeStruct((3, CONV_TAPS, 8, model_dim), F32)]
    ins = [*projs, tails, taps, logits, d_attn, q_act, k_act, t_mat, s_mat, r_mat, d_mat]
    return pl.pallas_call(
        functools.partial(backward_kernel, groups),
        grid=(n_seqs,),
        out_shape=outs,
        in_specs=[seq_block(arr.shape) for arr in ins[:4]] + [whole_block(taps.shape)] + [seq_block(arr.shape) for arr in ins[5:]],
        out_specs=[seq_block(out.shape) for out in outs[:-1]] + [whole_block(outs[-1].shape)],
        scratch_shapes=[
            pltpu.VMEM((n_seqs, n_heads, HEAD_DIM, HEAD_DIM), F32),
            pltpu.VMEM((SEND_SLOTS, n_heads, HEAD_DIM, HEAD_DIM), F32),
            pltpu.VMEM((n_seqs, 3, 8, model_dim), F32),
            pltpu.VMEM((SEND_SLOTS, 3, 8, model_dim), F32),
            pltpu.VMEM((3, seq_dev + 8, model_dim), F32),
            pltpu.VMEM((3, seq_dev + 8, model_dim), F32),
            pltpu.VMEM((3, n_heads, seq_dev, HEAD_DIM), BF16),
            pltpu.SemaphoreType.DMA((SEND_SLOTS,)),
            pltpu.SemaphoreType.DMA((n_seqs,)),
            pltpu.SemaphoreType.DMA((SEND_SLOTS,)),
            pltpu.SemaphoreType.DMA((n_seqs,)),
        ],
        compiler_params=pltpu.CompilerParams(collective_id=1, has_side_effects=True, vmem_limit_bytes=VMEM_LIMIT, dimension_semantics=('arbitrary',)),
        cost_estimate=pl.CostEstimate(flops=250_000_000_000, bytes_accessed=120_000_000, transcendentals=0),
        name='delta_backward',
    )(*ins)


def solution(mesh):
    groups = mesh.shape['sp']
    to_next = [(source, source + 1) for source in range(groups - 1)]
    seq_spec = P('dp', 'sp', None)
    full_mat = P(None, None)
    part_mat = P('dp', None)

    def local_step(x_in, dy_out, w_query, w_key, w_value, w_beta, conv_query, conv_key, conv_value, w_gate, norm_weight, w_out):
        seq_dev = x_in.shape[1]
        projs = [project(x_in, weight).astype(BF16) for weight in (w_query, w_key, w_value)]
        tails = lax.ppermute(jnp.concatenate([proj[:, seq_dev - PAD:] for proj in projs], axis=-1), 'sp', to_next)
        taps = jnp.stack([conv_query, conv_key, conv_value]).astype(F32)
        logits = project(x_in, w_beta).astype(BF16)
        gate_pre = project(x_in, w_gate).astype(BF16)
        d_hidden = back_project(dy_out, w_out).astype(BF16)
        norm_f = norm_weight.astype(F32).reshape(1, HEAD_DIM)
        hidden, d_gate, d_attn, q_act, k_act, t_mat, s_mat, r_mat, d_mat, dnorm = run_forward(groups, projs, tails, taps, logits, gate_pre, d_hidden, norm_f)
        y_out = project(hidden, w_out).astype(BF16)
        early = lax.psum((weight_grad(x_in, d_gate), weight_grad(hidden, dy_out)), 'sp')
        dp_q, dp_k, dp_v, d_logit, dtaps = run_backward(groups, projs, tails, taps, logits, d_attn, q_act, k_act, t_mat, s_mat, r_mat, d_mat)
        dtaps = jnp.sum(dtaps, axis=2)
        late_parts = (weight_grad(x_in, dp_q), weight_grad(x_in, dp_k), weight_grad(x_in, dp_v), weight_grad(x_in, d_logit), dtaps, jnp.sum(dnorm, axis=0))
        late_parts, early = lax.optimization_barrier((late_parts, early))
        late = lax.psum(late_parts, 'sp')
        dx_acc = back_project(d_gate, w_gate) + back_project(d_logit, w_beta) + back_project(dp_q, w_query) + back_project(dp_k, w_key) + back_project(dp_v, w_value)
        return (y_out, dx_acc.astype(BF16), late[0], late[1], late[2], late[3], late[4][0], late[4][1], late[4][2], early[0], late[5], early[1])

    in_specs = (seq_spec, seq_spec) + (full_mat,) * 8 + (P(None), full_mat)
    out_specs = (seq_spec, seq_spec) + (part_mat,) * 8 + (P('dp'), part_mat)
    return jax.shard_map(local_step, mesh=mesh, in_specs=in_specs, out_specs=out_specs, check_vma=False)
```

```python
import functools
import jax
import jax.numpy as jnp
from jax import lax
from jax.experimental import pallas as pl
from jax.experimental.pallas import tpu as pltpu
from jax.sharding import PartitionSpec as P

HEAD_DIM = 128
CONV_TAPS = 4
PAD = CONV_TAPS - 1
SEND_SLOTS = 4
CHUNK = 64
LAG_JOIN = 2
LAG_TOTAL = 5
LAG_END = 9
F32 = jnp.float32
BF16 = jnp.bfloat16
MESH = pl.DeviceIdType.MESH
VMEM_LIMIT = 60 * 1024 * 1024


def project(act_in, weight):
    return jnp.einsum('btd,de->bte', act_in, weight, preferred_element_type=F32)


def back_project(grad_in, weight):
    return jnp.einsum('bte,de->btd', grad_in, weight, preferred_element_type=F32)


def weight_grad(act_in, grad_in):
    return jnp.einsum('btd,bte->de', act_in, grad_in, preferred_element_type=F32)


def bdot(lhs, rhs, lhs_dim, rhs_dim):
    return lax.dot_general(lhs, rhs, (((lhs_dim,), (rhs_dim,)), ((0,), (0,))), preferred_element_type=F32)


def split(value):
    high = value.astype(BF16)
    return high, (value - high.astype(F32)).astype(BF16)


def dot_er(lhs, rhs, lhs_dim, rhs_dim):
    return bdot(lhs, rhs[0], lhs_dim, rhs_dim) + bdot(lhs, rhs[1], lhs_dim, rhs_dim)


def dot_re(lhs, rhs, lhs_dim, rhs_dim):
    return bdot(lhs[0], rhs, lhs_dim, rhs_dim) + bdot(lhs[1], rhs, lhs_dim, rhs_dim)


def dot_rr(lhs, rhs, lhs_dim, rhs_dim):
    return bdot(lhs[0], rhs[0], lhs_dim, rhs_dim) + (bdot(lhs[0], rhs[1], lhs_dim, rhs_dim) + bdot(lhs[1], rhs[0], lhs_dim, rhs_dim))


def block_inverse(low_mat, row_idx, col_idx):
    size = low_mat.shape[-1]
    eye = (row_idx == col_idx).astype(F32)
    low_split = split(low_mat)
    inv = eye - jnp.where(row_idx // 2 == col_idx // 2, low_mat, 0.0)
    width = 2
    while width < size:
        fresh = (row_idx // (2 * width) == col_idx // (2 * width)) & (row_idx // width != col_idx // width)
        corner = jnp.where(fresh, low_mat, 0.0).astype(BF16)
        inv_b = inv.astype(BF16)
        inv = inv - bdot(bdot(inv_b, corner, 2, 1).astype(BF16), inv_b, 2, 1)
        width *= 2
    inv_split = split(inv)
    resid = eye - inv - dot_rr(low_split, inv_split, 2, 1)
    return inv + bdot(inv_split[0], resid.astype(BF16), 2, 1)


def head_cols(head):
    return pl.ds(pl.multiple_of(head * HEAD_DIM, HEAD_DIM), HEAD_DIM)


def head_columns(array_in, n_heads):
    return jnp.concatenate([array_in[:, head:head + 1][None] for head in range(n_heads)], axis=0)


def entry_barrier(me, groups):
    barrier = pltpu.get_barrier_semaphore()
    for step in (1, groups - 1):
        pl.semaphore_signal(barrier, inc=1, device_id={'sp': lax.rem(me + step, groups)}, device_id_type=MESH)
    pl.semaphore_wait(barrier, 2)


def conv_rows(ext_ref, branch, cols, taps, seq_dev):
    total = ext_ref[branch, pl.ds(8 - PAD, seq_dev), cols] * taps[0:1]
    for tap_idx in range(1, CONV_TAPS):
        total = total + ext_ref[branch, pl.ds(8 - PAD + tap_idx, seq_dev), cols] * taps[tap_idx:tap_idx + 1]
    return total


def fill_ext(ext_ref, p_refs, tail_ref, cols, head, model_dim):
    seq_dev = p_refs[0].shape[1]
    for branch in range(3):
        tail_cols = pl.ds(pl.multiple_of(branch * model_dim + head * HEAD_DIM, HEAD_DIM), HEAD_DIM)
        ext_ref[branch, pl.ds(8 - PAD, PAD), cols] = tail_ref[0, :, tail_cols].astype(F32)
        ext_ref[branch, pl.ds(8, seq_dev), cols] = p_refs[branch][0, :, cols].astype(F32)


def forward_kernel(groups, pq_ref, pk_ref, pv_ref, tail_ref, taps_ref, logit_ref, z_ref, dh_ref, norm_ref,
                   h_ref, dz_ref, do_ref, q_ref, k_ref, t_ref, s_ref, r_ref, d_ref, dnorm_ref,
                   recv, send, ext, v_buf, o_buf, send_sem, recv_sem):
    step = pl.program_id(0)
    n_steps = pl.num_programs(0)
    me = lax.axis_index('sp')
    seq_dev = pq_ref.shape[1]
    model_dim = pq_ref.shape[2]
    n_heads = model_dim // HEAD_DIM
    slot = lax.rem(step, SEND_SLOTS)

    def hop(slot_idx, step_idx):
        return pltpu.make_async_remote_copy(
            src_ref=send.at[slot_idx], dst_ref=recv.at[step_idx], send_sem=send_sem.at[slot_idx], recv_sem=recv_sem.at[step_idx],
            device_id={'sp': lax.rem(me + 1, groups)}, device_id_type=MESH)

    @pl.when(step == 0)
    def _():
        entry_barrier(me, groups)
        dnorm_ref[...] = jnp.zeros_like(dnorm_ref)

    def act_head(head, carry):
        cols = head_cols(head)
        fill_ext(ext, (pq_ref, pk_ref, pv_ref), tail_ref, cols, head, model_dim)
        for branch in range(3):
            act = jax.nn.silu(conv_rows(ext, branch, cols, taps_ref[branch, :, cols], seq_dev))
            if branch < 2:
                act = act * lax.rsqrt(jnp.sum(act * act, axis=-1, keepdims=True) + 1e-6)
                (q_ref, k_ref)[branch][0, head] = act.astype(BF16)
            else:
                v_buf[head] = act.astype(BF16)
        return carry

    lax.fori_loop(0, n_heads, act_head, 0)

    beta = jax.nn.sigmoid(logit_ref[0].astype(F32)).astype(BF16).astype(F32)
    beta3 = head_columns(beta, n_heads)
    q_all = q_ref[0]
    k_all = k_ref[0]
    row_idx = lax.broadcasted_iota(jnp.int32, (1, seq_dev, seq_dev), 1)
    col_idx = lax.broadcasted_iota(jnp.int32, (1, seq_dev, seq_dev), 2)
    gram = bdot(k_all, k_all, 2, 2)
    t_ref[0] = block_inverse(jnp.where(row_idx > col_idx, beta3 * gram, 0.0), row_idx, col_idx)

    @pl.when(me > 0)
    def _():
        hop(slot, step).wait_recv()

    @pl.when(me == 0)
    def _():
        recv[step] = jnp.zeros(recv.shape[1:], F32)

    @pl.when((me < groups - 1) & (step >= SEND_SLOTS))
    def _():
        hop(slot, step).wait_send()

    state = recv[step]
    s_ref[0] = state
    state_split = split(state)
    resid = v_buf[...].astype(F32) - dot_er(k_all, state_split, 2, 1)
    r_ref[0] = resid
    delta = dot_rr(split(t_ref[0]), split(beta3 * resid), 2, 1)
    d_ref[0] = delta
    delta_split = split(delta)
    send[slot] = state + dot_er(k_all, delta_split, 1, 1)
    scores = jnp.where(row_idx >= col_idx, bdot(q_all, k_all, 2, 2), 0.0)
    o_buf[...] = (dot_er(q_all, state_split, 2, 1) + dot_rr(split(scores), delta_split, 2, 1)).astype(BF16).astype(F32)

    @pl.when(me < groups - 1)
    def _():
        hop(slot, step).start()

    def post_head(head, carry):
        cols = head_cols(head)
        attn = o_buf[head]
        norm_w = norm_ref[...]
        z_in = z_ref[0, :, cols].astype(F32)
        dh_in = dh_ref[0, :, cols].astype(F32)
        inv_rms = lax.rsqrt(jnp.mean(attn * attn, axis=-1, keepdims=True) + 1e-5)
        unit = attn * inv_rms
        normed = unit * norm_w
        sig = jax.nn.sigmoid(z_in)
        gate = z_in * sig
        h_ref[0, :, cols] = (normed * gate).astype(BF16)
        d_normed = dh_in * gate
        dz_ref[0, :, cols] = (dh_in * normed * (sig * (1.0 + z_in * (1.0 - sig)))).astype(BF16)
        d_unit = d_normed * norm_w
        dnorm_ref[...] += jnp.sum((d_normed * unit).reshape(seq_dev // 8, 8, HEAD_DIM), axis=0)
        do_ref[0, head] = (inv_rms * (d_unit - unit * jnp.mean(unit * d_unit, axis=-1, keepdims=True))).astype(BF16)
        return carry

    lax.fori_loop(0, n_heads, post_head, 0)

    @pl.when((me < groups - 1) & (step == n_steps - 1))
    def _():
        for back in range(min(SEND_SLOTS, recv.shape[0])):
            last = recv.shape[0] - 1 - back
            hop(last % SEND_SLOTS, last).wait_send()


def backward_kernel(groups, pq_ref, pk_ref, pv_ref, tail_ref, taps_ref, logit_ref, do_ref, q_ref, k_ref, t_ref, s_ref, r_ref, d_ref,
                    dpq_ref, dpk_ref, dpv_ref, dlogit_ref, dtaps_ref,
                    recv, send, front, front_send, ext, dext, dact, send_sem, recv_sem, fsend_sem, frecv_sem):
    step = pl.program_id(0)
    n_steps = pl.num_programs(0)
    me = lax.axis_index('sp')
    seq_dev = pq_ref.shape[1]
    model_dim = pq_ref.shape[2]
    n_heads = model_dim // HEAD_DIM
    slot = lax.rem(step, SEND_SLOTS)
    to_prev = lax.rem(me + groups - 1, groups)

    def hop(slot_idx, step_idx):
        return pltpu.make_async_remote_copy(
            src_ref=send.at[slot_idx], dst_ref=recv.at[step_idx], send_sem=send_sem.at[slot_idx], recv_sem=recv_sem.at[step_idx],
            device_id={'sp': to_prev}, device_id_type=MESH)

    def front_hop(slot_idx, step_idx):
        return pltpu.make_async_remote_copy(
            src_ref=front_send.at[slot_idx], dst_ref=front.at[step_idx], send_sem=fsend_sem.at[slot_idx], recv_sem=frecv_sem.at[step_idx],
            device_id={'sp': to_prev}, device_id_type=MESH)

    @pl.when(step == 0)
    def _():
        entry_barrier(me, groups)
        dtaps_ref[...] = jnp.zeros_like(dtaps_ref)

    sig_beta = jax.nn.sigmoid(logit_ref[0].astype(F32))
    beta3 = head_columns(sig_beta.astype(BF16).astype(F32), n_heads)
    q_all = q_ref[0]
    k_all = k_ref[0]
    d_out = do_ref[0]
    row_idx = lax.broadcasted_iota(jnp.int32, (1, seq_dev, seq_dev), 1)
    col_idx = lax.broadcasted_iota(jnp.int32, (1, seq_dev, seq_dev), 2)
    gram = bdot(k_all, k_all, 2, 2)
    scores = jnp.where(row_idx >= col_idx, bdot(q_all, k_all, 2, 2), 0.0)
    t_split = split(t_ref[0])
    delta_split = split(d_ref[0])
    state_split = split(s_ref[0])
    d_delta_own = dot_re(split(scores), d_out, 1, 1)
    state_own = bdot(q_all, d_out, 1, 1)
    d_scores = jnp.where(row_idx >= col_idx, dot_er(d_out, delta_split, 2, 2), 0.0).astype(BF16)
    dact[0] = (dot_er(d_out, state_split, 2, 2) + bdot(d_scores, k_all, 2, 1)).astype(BF16)

    @pl.when(me < groups - 1)
    def _():
        hop(slot, step).wait_recv()

    @pl.when(me == groups - 1)
    def _():
        recv[step] = jnp.zeros(recv.shape[1:], F32)
        front[step] = jnp.zeros(front.shape[1:], F32)

    @pl.when((me > 0) & (step >= SEND_SLOTS))
    def _():
        hop(slot, step).wait_send()
        front_hop(slot, step).wait_send()

    d_state = recv[step]
    d_state_split = split(d_state)
    d_delta = d_delta_own + dot_er(k_all, d_state_split, 2, 1)
    d_rhs = dot_rr(t_split, split(d_delta), 1, 1)
    d_resid = beta3 * d_rhs
    d_resid_split = split(d_resid)
    send[slot] = d_state + state_own - dot_er(k_all, d_resid_split, 1, 1)
    dact[2] = d_resid.astype(BF16)
    d_low = jnp.where(row_idx > col_idx, -dot_rr(split(d_rhs), delta_split, 2, 2), 0.0)
    d_beta = jnp.sum(d_rhs * r_ref[0], axis=-1, keepdims=True) + jnp.sum(d_low * gram, axis=-1, keepdims=True)
    d_gram = (beta3 * d_low).astype(BF16)
    d_key = dot_rr(delta_split, d_state_split, 2, 2) - dot_rr(d_resid_split, state_split, 2, 2)
    d_key = d_key + bdot(d_gram, k_all, 2, 1) + bdot(d_gram, k_all, 1, 1) + bdot(d_scores, q_all, 1, 1)
    dact[1] = d_key.astype(BF16)
    lane_idx = lax.broadcasted_iota(jnp.int32, (seq_dev, n_heads), 1)
    beta_grad = jnp.zeros((seq_dev, n_heads), F32)
    for head in range(n_heads):
        beta_grad = beta_grad + jnp.where(lane_idx == head, d_beta[head], 0.0)
    dlogit_ref[0] = (beta_grad.astype(BF16).astype(F32) * sig_beta * (1.0 - sig_beta)).astype(BF16)

    @pl.when(me > 0)
    def _():
        hop(slot, step).start()

    def act_head(head, carry):
        cols = head_cols(head)
        fill_ext(ext, (pq_ref, pk_ref, pv_ref), tail_ref, cols, head, model_dim)
        for branch in range(3):
            conv_sum = conv_rows(ext, branch, cols, taps_ref[branch, :, cols], seq_dev)
            sig = jax.nn.sigmoid(conv_sum)
            d_act = dact[branch, head].astype(F32)
            if branch < 2:
                act = conv_sum * sig
                inv_norm = lax.rsqrt(jnp.sum(act * act, axis=-1, keepdims=True) + 1e-6)
                unit = act * inv_norm
                d_act = inv_norm * (d_act - unit * jnp.sum(unit * d_act, axis=-1, keepdims=True))
            d_conv = d_act * (sig * (1.0 + conv_sum * (1.0 - sig)))
            dext[branch, pl.ds(0, seq_dev), cols] = d_conv
            front_send[slot, branch, :, cols] = d_conv[0:8]
            for tap_idx in range(CONV_TAPS):
                prod = d_conv * ext[branch, pl.ds(8 - PAD + tap_idx, seq_dev), cols]
                dtaps_ref[branch, tap_idx, :, cols] += jnp.sum(prod.reshape(seq_dev // 8, 8, HEAD_DIM), axis=0)
        return carry

    lax.fori_loop(0, n_heads, act_head, 0)

    @pl.when(me > 0)
    def _():
        front_hop(slot, step).start()

    @pl.when(me < groups - 1)
    def _():
        front_hop(slot, step).wait_recv()

    def conv_head(head, carry):
        cols = head_cols(head)
        for branch in range(3):
            taps = taps_ref[branch, :, cols]
            dext[branch, pl.ds(seq_dev, 8), cols] = front[step, branch, :, cols]
            total = dext[branch, pl.ds(PAD, seq_dev), cols] * taps[0:1]
            for tap_idx in range(1, CONV_TAPS):
                total = total + dext[branch, pl.ds(PAD - tap_idx, seq_dev), cols] * taps[tap_idx:tap_idx + 1]
            (dpq_ref, dpk_ref, dpv_ref)[branch][0, :, cols] = total.astype(BF16)
        return carry

    lax.fori_loop(0, n_heads, conv_head, 0)

    @pl.when((me > 0) & (step == n_steps - 1))
    def _():
        for back in range(min(SEND_SLOTS, recv.shape[0])):
            last = recv.shape[0] - 1 - back
            hop(last % SEND_SLOTS, last).wait_send()
            front_hop(last % SEND_SLOTS, last).wait_send()


def seq_block(shape):
    return pl.BlockSpec((1,) + tuple(shape[1:]), lambda step: (step,) + (0,) * (len(shape) - 1))


def whole_block(shape):
    return pl.BlockSpec(tuple(shape), lambda step: (0,) * len(shape))


def run_forward(groups, projs, tails, taps, logits, gate_pre, d_hidden, norm_f):
    n_seqs, seq_dev, model_dim = gate_pre.shape
    n_heads = model_dim // HEAD_DIM
    tok = jax.ShapeDtypeStruct((n_seqs, seq_dev, model_dim), BF16)
    per_head_b = jax.ShapeDtypeStruct((n_seqs, n_heads, seq_dev, HEAD_DIM), BF16)
    per_head_f = jax.ShapeDtypeStruct((n_seqs, n_heads, seq_dev, HEAD_DIM), F32)
    outs = [tok, tok, per_head_b, per_head_b, per_head_b,
            jax.ShapeDtypeStruct((n_seqs, n_heads, seq_dev, seq_dev), F32),
            jax.ShapeDtypeStruct((n_seqs, n_heads, HEAD_DIM, HEAD_DIM), F32),
            per_head_f, per_head_f, jax.ShapeDtypeStruct((8, HEAD_DIM), F32)]
    ins = [*projs, tails, taps, logits, gate_pre, d_hidden, norm_f]
    return pl.pallas_call(
        functools.partial(forward_kernel, groups),
        grid=(n_seqs,),
        out_shape=outs,
        in_specs=[seq_block(arr.shape) for arr in ins[:4]] + [whole_block(taps.shape)] + [seq_block(arr.shape) for arr in ins[5:8]] + [whole_block(norm_f.shape)],
        out_specs=[seq_block(out.shape) for out in outs[:-1]] + [whole_block(outs[-1].shape)],
        scratch_shapes=[
            pltpu.VMEM((n_seqs, n_heads, HEAD_DIM, HEAD_DIM), F32),
            pltpu.VMEM((SEND_SLOTS, n_heads, HEAD_DIM, HEAD_DIM), F32),
            pltpu.VMEM((3, seq_dev + 8, model_dim), F32),
            pltpu.VMEM((n_heads, seq_dev, HEAD_DIM), BF16),
            pltpu.VMEM((n_heads, seq_dev, HEAD_DIM), F32),
            pltpu.SemaphoreType.DMA((SEND_SLOTS,)),
            pltpu.SemaphoreType.DMA((n_seqs,)),
        ],
        compiler_params=pltpu.CompilerParams(collective_id=0, has_side_effects=True, vmem_limit_bytes=VMEM_LIMIT, dimension_semantics=('arbitrary',)),
        cost_estimate=pl.CostEstimate(flops=200_000_000_000, bytes_accessed=120_000_000, transcendentals=0),
        name='delta_forward',
    )(*ins)


def run_backward(groups, projs, tails, taps, logits, d_attn, q_act, k_act, t_mat, s_mat, r_mat, d_mat):
    n_seqs, seq_dev, model_dim = projs[0].shape
    n_heads = model_dim // HEAD_DIM
    tok = jax.ShapeDtypeStruct((n_seqs, seq_dev, model_dim), BF16)
    outs = [tok, tok, tok, jax.ShapeDtypeStruct(logits.shape, BF16), jax.ShapeDtypeStruct((3, CONV_TAPS, 8, model_dim), F32)]
    ins = [*projs, tails, taps, logits, d_attn, q_act, k_act, t_mat, s_mat, r_mat, d_mat]
    return pl.pallas_call(
        functools.partial(backward_kernel, groups),
        grid=(n_seqs,),
        out_shape=outs,
        in_specs=[seq_block(arr.shape) for arr in ins[:4]] + [whole_block(taps.shape)] + [seq_block(arr.shape) for arr in ins[5:]],
        out_specs=[seq_block(out.shape) for out in outs[:-1]] + [whole_block(outs[-1].shape)],
        scratch_shapes=[
            pltpu.VMEM((n_seqs, n_heads, HEAD_DIM, HEAD_DIM), F32),
            pltpu.VMEM((SEND_SLOTS, n_heads, HEAD_DIM, HEAD_DIM), F32),
            pltpu.VMEM((n_seqs, 3, 8, model_dim), F32),
            pltpu.VMEM((SEND_SLOTS, 3, 8, model_dim), F32),
            pltpu.VMEM((3, seq_dev + 8, model_dim), F32),
            pltpu.VMEM((3, seq_dev + 8, model_dim), F32),
            pltpu.VMEM((3, n_heads, seq_dev, HEAD_DIM), BF16),
            pltpu.SemaphoreType.DMA((SEND_SLOTS,)),
            pltpu.SemaphoreType.DMA((n_seqs,)),
            pltpu.SemaphoreType.DMA((SEND_SLOTS,)),
            pltpu.SemaphoreType.DMA((n_seqs,)),
        ],
        compiler_params=pltpu.CompilerParams(collective_id=1, has_side_effects=True, vmem_limit_bytes=VMEM_LIMIT, dimension_semantics=('arbitrary',)),
        cost_estimate=pl.CostEstimate(flops=250_000_000_000, bytes_accessed=120_000_000, transcendentals=0),
        name='delta_backward',
    )(*ins)


def tail_kernel(n_seqs, *refs):
    parts, (h_ref, dg_ref, dq_ref, dk_ref, dv_ref, dl_ref), (wo_ref, wg_ref, wq_ref, wk_ref, wv_ref, wb_ref) = refs[:6], refs[6:12], refs[12:18]
    sums, (y_ref, dx_ref) = refs[18:24], refs[24:26]
    own, pair, outer, inner, load_sem, psend, precv, osend, orecv, isend, irecv, store_sem, csend, crecv = refs[26:]
    step = pl.program_id(0)
    n_chunks = own.shape[0] // CHUNK
    last_step = n_chunks + LAG_END
    me = lax.axis_index('sp')
    chip = me // 2
    core = lax.rem(me, 2)
    partner = me + 1 - 2 * core
    is_end = (chip == 0) | (chip == 3)
    is_mid = (chip == 1) | (chip == 2)
    outer_dev = lax.rem(me + 8 + 2 - 4 * lax.rem(chip, 2), 8)
    inner_dev = lax.rem(me + 8 - 2 + 4 * lax.rem(chip, 2), 8)
    group_len = parts[0].shape[0] // 2 // CHUNK

    def rows(idx):
        return pl.ds(pl.multiple_of(idx * CHUNK, CHUNK), CHUNK)

    def half(idx, which):
        size = parts[idx].shape[0] // 2
        return pl.ds(pl.multiple_of(which * size, CHUNK), size)

    def buf_rows(idx):
        return pl.ds(idx * group_len * CHUNK, parts[idx].shape[0] // 2)

    def remote(src, dst, send_sem, recv_sem, dev):
        return pltpu.make_async_remote_copy(src_ref=src, dst_ref=dst, send_sem=send_sem, recv_sem=recv_sem, device_id={'sp': dev}, device_id_type=MESH)

    def load_copy(idx):
        return pltpu.make_async_copy(parts[idx].at[half(idx, core)], own.at[buf_rows(idx)], load_sem.at[idx])

    def pair_copy(idx):
        return remote(parts[idx].at[half(idx, 1 - core)], pair.at[buf_rows(idx)], psend.at[idx], precv.at[idx], partner)

    def outer_copy(src, idx):
        return remote(src.at[rows(idx)], outer.at[rows(idx)], osend.at[idx], orecv.at[idx], outer_dev)

    def inner_copy(idx):
        return remote(own.at[rows(idx)], inner.at[rows(idx)], isend.at[idx], irecv.at[idx], inner_dev)

    def store_copy(src, idx):
        return pltpu.make_async_copy(src.at[buf_rows(idx)], sums[idx].at[half(idx, core)], store_sem.at[idx])

    def give_copy(src, idx):
        return remote(src.at[buf_rows(idx)], sums[idx].at[half(idx, core)], csend.at[idx], crecv.at[idx], partner)

    @pl.when(step == 0)
    def _():
        barrier = pltpu.get_barrier_semaphore()
        for other in range(1, 8):
            pl.semaphore_signal(barrier, inc=1, device_id={'sp': lax.rem(me + other, 8)}, device_id_type=MESH)
        pl.semaphore_wait(barrier, 7)
        for idx in range(len(parts)):
            load_copy(idx).start()
            pair_copy(idx).start()

    @pl.when(is_end & (step >= 1) & (step <= n_chunks))
    def _():
        outer_copy(own, step - 1).start()

    @pl.when(is_mid & (step >= LAG_JOIN + 1) & (step <= n_chunks + LAG_JOIN))
    def _():
        inner_copy(step - LAG_JOIN - 1).start()

    @pl.when(is_mid & (step >= LAG_TOTAL + 1) & (step <= n_chunks + LAG_TOTAL))
    def _():
        outer_copy(pair, step - LAG_TOTAL - 1).start()

    for idx in range(len(parts)):
        final = idx * group_len + parts[idx].shape[0] // 2 // CHUNK - 1

        @pl.when(is_mid & (step == final + LAG_TOTAL + 1))
        def _():
            store_copy(pair, idx).start()
            give_copy(pair, idx).start()

        @pl.when(step == idx * group_len)
        def _():
            load_copy(idx).wait()
            pair_copy(idx).wait_recv()

    @pl.when(step < n_seqs)
    def _():
        y_ref[0] = lax.dot_general(h_ref[0], wo_ref[...], (((1,), (0,)), ((), ())), preferred_element_type=F32).astype(BF16)
        total = lax.dot_general(dg_ref[0], wg_ref[...], (((1,), (1,)), ((), ())), preferred_element_type=F32)
        for grad_ref, w_ref in ((dl_ref, wb_ref), (dq_ref, wq_ref), (dk_ref, wk_ref), (dv_ref, wv_ref)):
            total = total + lax.dot_general(grad_ref[0], w_ref[...], (((1,), (1,)), ((), ())), preferred_element_type=F32)
        dx_ref[0] = total.astype(BF16)

    @pl.when(step < n_chunks)
    def _():
        own[rows(step)] = own[rows(step)] + pair[rows(step)]

    @pl.when(is_mid & (step >= LAG_JOIN) & (step < n_chunks + LAG_JOIN))
    def _():
        idx = step - LAG_JOIN
        outer_copy(pair, idx).wait_recv()
        own[rows(idx)] = own[rows(idx)] + outer[rows(idx)]

    @pl.when(is_mid & (step >= LAG_TOTAL) & (step < n_chunks + LAG_TOTAL))
    def _():
        idx = step - LAG_TOTAL
        inner_copy(idx).wait_recv()
        pair[rows(idx)] = own[rows(idx)] + inner[rows(idx)]

    @pl.when(is_end & (step >= LAG_END) & (step < n_chunks + LAG_END))
    def _():
        outer_copy(own, step - LAG_END).wait_recv()

    for idx in range(len(parts)):
        final = idx * group_len + parts[idx].shape[0] // 2 // CHUNK - 1

        @pl.when(is_end & (step == final + LAG_END))
        def _():
            store_copy(outer, idx).start()
            give_copy(outer, idx).start()

    @pl.when(step == last_step)
    def _():
        for idx in range(len(parts)):
            pair_copy(idx).wait_send()
            store_copy(outer, idx).wait()
            give_copy(outer, idx).wait()

        def drain_outer(idx, carry):
            outer_copy(own, idx).wait_send()
            return carry

        lax.fori_loop(0, n_chunks, drain_outer, 0)

        @pl.when(is_mid)
        def _():
            def drain_inner(idx, carry):
                inner_copy(idx).wait_send()
                return carry

            lax.fori_loop(0, n_chunks, drain_inner, 0)


def run_tail(parts, acts, weights):
    n_seqs, seq_dev, model_dim = acts[0].shape
    n_rows = sum(part.shape[0] for part in parts) // 2
    n_chunks = n_rows // CHUNK
    n_parts = len(parts)
    any_spec = pl.BlockSpec(memory_space=pl.ANY)

    def row_block(arr):
        return pl.BlockSpec((1,) + tuple(arr.shape[1:]), lambda step: (jnp.minimum(step, n_seqs - 1), 0, 0))

    outs = [jax.ShapeDtypeStruct(part.shape, F32) for part in parts] + [jax.ShapeDtypeStruct(acts[0].shape, BF16)] * 2
    buf = pltpu.VMEM((n_rows, model_dim), F32)
    part_sems = pltpu.SemaphoreType.DMA((n_parts,))
    chunk_sems = pltpu.SemaphoreType.DMA((n_chunks,))
    return pl.pallas_call(
        functools.partial(tail_kernel, n_seqs),
        grid=(n_chunks + LAG_END + 1,),
        out_shape=outs,
        in_specs=[any_spec] * n_parts + [row_block(arr) for arr in acts] + [pl.BlockSpec(memory_space=pltpu.VMEM) for _ in weights],
        out_specs=[any_spec] * n_parts + [row_block(acts[0])] * 2,
        scratch_shapes=[buf] * 4 + [part_sems] * 3 + [chunk_sems] * 4 + [part_sems] * 3,
        compiler_params=pltpu.CompilerParams(collective_id=2, has_side_effects=True, vmem_limit_bytes=62 * 1024 * 1024, dimension_semantics=('arbitrary',)),
        cost_estimate=pl.CostEstimate(flops=250_000_000_000, bytes_accessed=120_000_000, transcendentals=0),
        name='sum_and_project',
    )(*parts, *acts, *weights)


def solution(mesh):
    groups = mesh.shape['sp']
    to_next = [(source, source + 1) for source in range(groups - 1)]
    seq_spec = P('dp', 'sp', None)
    full_mat = P(None, None)
    part_mat = P('dp', None)

    def local_step(x_in, dy_out, w_query, w_key, w_value, w_beta, conv_query, conv_key, conv_value, w_gate, norm_weight, w_out):
        seq_dev = x_in.shape[1]
        projs = [project(x_in, weight).astype(BF16) for weight in (w_query, w_key, w_value)]
        tails = lax.ppermute(jnp.concatenate([proj[:, seq_dev - PAD:] for proj in projs], axis=-1), 'sp', to_next)
        taps = jnp.stack([conv_query, conv_key, conv_value]).astype(F32)
        logits = project(x_in, w_beta).astype(BF16)
        gate_pre = project(x_in, w_gate).astype(BF16)
        d_hidden = back_project(dy_out, w_out).astype(BF16)
        norm_f = norm_weight.astype(F32).reshape(1, HEAD_DIM)
        hidden, d_gate, d_attn, q_act, k_act, t_mat, s_mat, r_mat, d_mat, dnorm = run_forward(groups, projs, tails, taps, logits, gate_pre, d_hidden, norm_f)
        dp_q, dp_k, dp_v, d_logit, dtaps = run_backward(groups, projs, tails, taps, logits, d_attn, q_act, k_act, t_mat, s_mat, r_mat, d_mat)
        model_dim = x_in.shape[2]
        small = jnp.concatenate([
            jnp.einsum('bte,btd->ed', d_logit, x_in, preferred_element_type=F32),
            jnp.sum(dtaps, axis=2).reshape(3 * CONV_TAPS, model_dim),
            jnp.pad(jnp.sum(dnorm, axis=0, keepdims=True), ((0, 0), (0, model_dim - HEAD_DIM)))])
        n_heads = w_beta.shape[1]
        small = jnp.pad(small, ((0, 2 * CHUNK - small.shape[0]), (0, 0)))
        grads = (weight_grad(x_in, d_gate), weight_grad(hidden, dy_out), weight_grad(x_in, dp_q), weight_grad(x_in, dp_k), weight_grad(x_in, dp_v), small)
        dw_gate, dw_out, dw_q, dw_k, dw_v, small, y_out, dx_in = run_tail(
            grads, (hidden, d_gate, dp_q, dp_k, dp_v, d_logit), (w_out, w_gate, w_query, w_key, w_value, w_beta))
        dtaps = small[n_heads:n_heads + 3 * CONV_TAPS].reshape(3, CONV_TAPS, model_dim)
        dnorm = small[n_heads + 3 * CONV_TAPS, :HEAD_DIM]
        return (y_out, dx_in, dw_q, dw_k, dw_v, small[:n_heads].T, dtaps[0], dtaps[1], dtaps[2], dw_gate, dnorm, dw_out)

    in_specs = (seq_spec, seq_spec) + (full_mat,) * 8 + (P(None), full_mat)
    out_specs = (seq_spec, seq_spec) + (part_mat,) * 8 + (P('dp'), part_mat)
    return jax.shard_map(local_step, mesh=mesh, in_specs=in_specs, out_specs=out_specs, check_vma=False)
```

```python
import functools
import jax
import jax.numpy as jnp
from jax import lax
from jax.experimental import pallas as pl
from jax.experimental.pallas import tpu as pltpu
from jax.sharding import PartitionSpec as P

HEAD_DIM = 128
CONV_TAPS = 4
PAD = CONV_TAPS - 1
SEND_SLOTS = 4
CHUNK = 64
LAG_JOIN = 2
LAG_TOTAL = 5
LAG_END = 9
F32 = jnp.float32
BF16 = jnp.bfloat16
MESH = pl.DeviceIdType.MESH
VMEM_LIMIT = 60 * 1024 * 1024


def project(act_in, weight):
    return jnp.einsum('btd,de->bte', act_in, weight, preferred_element_type=F32)


def back_project(grad_in, weight):
    return jnp.einsum('bte,de->btd', grad_in, weight, preferred_element_type=F32)


def weight_grad(act_in, grad_in):
    return jnp.einsum('btd,bte->de', act_in, grad_in, preferred_element_type=F32)


def bdot(lhs, rhs, lhs_dim, rhs_dim):
    return lax.dot_general(lhs, rhs, (((lhs_dim,), (rhs_dim,)), ((0,), (0,))), preferred_element_type=F32)


def split(value):
    high = value.astype(BF16)
    return high, (value - high.astype(F32)).astype(BF16)


def rows_cat(*parts):
    return jnp.concatenate(parts, axis=1)


def twice(value, axis):
    return jnp.concatenate([value, value], axis=axis)


def joined(pair, axis):
    return jnp.concatenate(pair, axis=axis)


def dot_er(lhs, rhs, lhs_dim, rhs_dim):
    if lhs_dim == 2 and lhs.shape[2] == HEAD_DIM:
        return bdot(twice(lhs, 2), joined(rhs, rhs_dim), 2, rhs_dim)
    return bdot(lhs, rhs[0], lhs_dim, rhs_dim) + bdot(lhs, rhs[1], lhs_dim, rhs_dim)


def dot_re(lhs, rhs, lhs_dim, rhs_dim):
    return bdot(lhs[0], rhs, lhs_dim, rhs_dim) + bdot(lhs[1], rhs, lhs_dim, rhs_dim)


def dot_rr(lhs, rhs, lhs_dim, rhs_dim):
    if lhs_dim == 2:
        n_rows = lhs[0].shape[1]
        both = rows_cat(*lhs)
        if both.shape[2] == HEAD_DIM:
            prod = bdot(twice(both, 2), joined(rhs, rhs_dim), 2, rhs_dim)
            return prod[:, :n_rows] + prod[:, n_rows:]
        prod = bdot(both, rhs[0], 2, rhs_dim)
        return prod[:, :n_rows] + (prod[:, n_rows:] + bdot(lhs[0], rhs[1], 2, rhs_dim))
    return bdot(lhs[0], rhs[0], lhs_dim, rhs_dim) + (bdot(lhs[0], rhs[1], lhs_dim, rhs_dim) + bdot(lhs[1], rhs[0], lhs_dim, rhs_dim))


def block_inverse(low_mat, row_idx, col_idx):
    size = low_mat.shape[-1]
    eye = (row_idx == col_idx).astype(F32)
    low_split = split(low_mat)
    inv = eye - jnp.where(row_idx // 2 == col_idx // 2, low_mat, 0.0)
    width = 2
    while width < size:
        fresh = (row_idx // (2 * width) == col_idx // (2 * width)) & (row_idx // width != col_idx // width)
        corner = jnp.where(fresh, low_mat, 0.0).astype(BF16)
        inv_b = inv.astype(BF16)
        inv = inv - bdot(bdot(inv_b, corner, 2, 1).astype(BF16), inv_b, 2, 1)
        width *= 2
    inv_split = split(inv)
    resid = eye - inv - dot_rr(low_split, inv_split, 2, 1)
    return inv + bdot(inv_split[0], resid.astype(BF16), 2, 1)


def head_cols(head):
    return pl.ds(pl.multiple_of(head * HEAD_DIM, HEAD_DIM), HEAD_DIM)


def head_columns(array_in, n_heads):
    return jnp.concatenate([array_in[:, head:head + 1][None] for head in range(n_heads)], axis=0)


def entry_barrier(me, groups):
    barrier = pltpu.get_barrier_semaphore()
    for step in (1, groups - 1):
        pl.semaphore_signal(barrier, inc=1, device_id={'sp': lax.rem(me + step, groups)}, device_id_type=MESH)
    pl.semaphore_wait(barrier, 2)


def conv_rows(ext_ref, branch, cols, taps, seq_dev):
    total = ext_ref[branch, pl.ds(8 - PAD, seq_dev), cols] * taps[0:1]
    for tap_idx in range(1, CONV_TAPS):
        total = total + ext_ref[branch, pl.ds(8 - PAD + tap_idx, seq_dev), cols] * taps[tap_idx:tap_idx + 1]
    return total


def fill_ext(ext_ref, p_refs, tail_ref, cols, head, model_dim):
    seq_dev = p_refs[0].shape[1]
    for branch in range(3):
        tail_cols = pl.ds(pl.multiple_of(branch * model_dim + head * HEAD_DIM, HEAD_DIM), HEAD_DIM)
        ext_ref[branch, pl.ds(8 - PAD, PAD), cols] = tail_ref[0, :, tail_cols].astype(F32)
        ext_ref[branch, pl.ds(8, seq_dev), cols] = p_refs[branch][0, :, cols].astype(F32)


def forward_kernel(groups, pq_ref, pk_ref, pv_ref, tail_ref, taps_ref, logit_ref, z_ref, dh_ref, norm_ref,
                   h_ref, dz_ref, do_ref, q_ref, k_ref, t_ref, s_ref, r_ref, d_ref, dnorm_ref,
                   recv, send, ext, v_buf, o_buf, score_buf, send_sem, recv_sem):
    step = pl.program_id(0)
    n_steps = pl.num_programs(0)
    me = lax.axis_index('sp')
    seq_dev = pq_ref.shape[1]
    model_dim = pq_ref.shape[2]
    n_heads = model_dim // HEAD_DIM
    slot = lax.rem(step, SEND_SLOTS)

    def hop(slot_idx, step_idx):
        return pltpu.make_async_remote_copy(
            src_ref=send.at[slot_idx], dst_ref=recv.at[step_idx], send_sem=send_sem.at[slot_idx], recv_sem=recv_sem.at[step_idx],
            device_id={'sp': lax.rem(me + 1, groups)}, device_id_type=MESH)

    @pl.when(step == 0)
    def _():
        entry_barrier(me, groups)
        dnorm_ref[...] = jnp.zeros_like(dnorm_ref)

        @pl.when(me == 0)
        def _():
            recv[0] = jnp.zeros(recv.shape[1:], F32)

    def act_head(head, carry):
        cols = head_cols(head)
        fill_ext(ext, (pq_ref, pk_ref, pv_ref), tail_ref, cols, head, model_dim)
        for branch in range(3):
            act = jax.nn.silu(conv_rows(ext, branch, cols, taps_ref[branch, :, cols], seq_dev))
            if branch < 2:
                act = act * lax.rsqrt(jnp.sum(act * act, axis=-1, keepdims=True) + 1e-6)
                (q_ref, k_ref)[branch][0, head] = act.astype(BF16)
            else:
                v_buf[head] = act.astype(BF16)
        return carry

    lax.fori_loop(0, n_heads, act_head, 0)

    beta = jax.nn.sigmoid(logit_ref[0].astype(F32)).astype(BF16).astype(F32)
    beta3 = head_columns(beta, n_heads)
    q_all = q_ref[0]
    k_all = k_ref[0]
    row_idx = lax.broadcasted_iota(jnp.int32, (1, seq_dev, seq_dev), 1)
    col_idx = lax.broadcasted_iota(jnp.int32, (1, seq_dev, seq_dev), 2)
    kq_all = rows_cat(k_all, q_all)
    kq_prod = bdot(kq_all, k_all, 2, 2)
    gram = kq_prod[:, :seq_dev]
    score_buf[...] = jnp.where(row_idx >= col_idx, kq_prod[:, seq_dev:], 0.0)
    t_ref[0] = block_inverse(jnp.where(row_idx > col_idx, beta3 * gram, 0.0), row_idx, col_idx)

    @pl.when(me > 0)
    def _():
        hop(slot, step).wait_recv()

    @pl.when((me < groups - 1) & (step >= SEND_SLOTS))
    def _():
        hop(slot, step).wait_send()

    state = recv[step * jnp.minimum(me, 1)]
    s_ref[0] = state
    kq_state = dot_er(rows_cat(k_ref[0], q_ref[0]), split(state), 2, 1)
    resid = v_buf[...].astype(F32) - kq_state[:, :seq_dev]
    r_ref[0] = resid
    delta = dot_rr(split(t_ref[0]), split(beta3 * resid), 2, 1)
    d_ref[0] = delta
    delta_split = split(delta)
    send[slot] = state + dot_er(k_ref[0], delta_split, 1, 1)
    o_buf[...] = (kq_state[:, seq_dev:] + dot_rr(split(score_buf[...]), delta_split, 2, 1)).astype(BF16).astype(F32)

    @pl.when(me < groups - 1)
    def _():
        hop(slot, step).start()

    def post_head(head, carry):
        cols = head_cols(head)
        attn = o_buf[head]
        norm_w = norm_ref[...]
        z_in = z_ref[0, :, cols].astype(F32)
        dh_in = dh_ref[0, :, cols].astype(F32)
        inv_rms = lax.rsqrt(jnp.mean(attn * attn, axis=-1, keepdims=True) + 1e-5)
        unit = attn * inv_rms
        normed = unit * norm_w
        sig = jax.nn.sigmoid(z_in)
        gate = z_in * sig
        h_ref[0, :, cols] = (normed * gate).astype(BF16)
        d_normed = dh_in * gate
        dz_ref[0, :, cols] = (dh_in * normed * (sig * (1.0 + z_in * (1.0 - sig)))).astype(BF16)
        d_unit = d_normed * norm_w
        dnorm_ref[...] += jnp.sum((d_normed * unit).reshape(seq_dev // 8, 8, HEAD_DIM), axis=0)
        do_ref[0, head] = (inv_rms * (d_unit - unit * jnp.mean(unit * d_unit, axis=-1, keepdims=True))).astype(BF16)
        return carry

    lax.fori_loop(0, n_heads, post_head, 0)

    @pl.when((me < groups - 1) & (step == n_steps - 1))
    def _():
        for back in range(min(SEND_SLOTS, recv.shape[0])):
            last = recv.shape[0] - 1 - back
            hop(last % SEND_SLOTS, last).wait_send()


def backward_kernel(groups, pq_ref, pk_ref, pv_ref, tail_ref, taps_ref, logit_ref, do_ref, q_ref, k_ref, t_ref, s_ref, r_ref, d_ref,
                    dpq_ref, dpk_ref, dpv_ref, dlogit_ref, dtaps_ref,
                    recv, send, front, front_send, ext, dext, dact, gram_buf, delta_buf, state_buf, rhs_buf, send_sem, recv_sem, fsend_sem, frecv_sem):
    step = pl.program_id(0)
    n_steps = pl.num_programs(0)
    me = lax.axis_index('sp')
    seq_dev = pq_ref.shape[1]
    model_dim = pq_ref.shape[2]
    n_heads = model_dim // HEAD_DIM
    slot = lax.rem(step, SEND_SLOTS)
    to_prev = lax.rem(me + groups - 1, groups)

    def hop(slot_idx, step_idx):
        return pltpu.make_async_remote_copy(
            src_ref=send.at[slot_idx], dst_ref=recv.at[step_idx], send_sem=send_sem.at[slot_idx], recv_sem=recv_sem.at[step_idx],
            device_id={'sp': to_prev}, device_id_type=MESH)

    def front_hop(slot_idx, step_idx):
        return pltpu.make_async_remote_copy(
            src_ref=front_send.at[slot_idx], dst_ref=front.at[step_idx], send_sem=fsend_sem.at[slot_idx], recv_sem=frecv_sem.at[step_idx],
            device_id={'sp': to_prev}, device_id_type=MESH)

    @pl.when(step == 0)
    def _():
        entry_barrier(me, groups)
        dtaps_ref[...] = jnp.zeros_like(dtaps_ref)

        @pl.when(me == groups - 1)
        def _():
            recv[0] = jnp.zeros(recv.shape[1:], F32)
            front[0] = jnp.zeros(front.shape[1:], F32)

    sig_beta = jax.nn.sigmoid(logit_ref[0].astype(F32))
    beta3 = head_columns(sig_beta.astype(BF16).astype(F32), n_heads)
    from_next = step * jnp.minimum(groups - 1 - me, 1)
    row_idx = lax.broadcasted_iota(jnp.int32, (1, seq_dev, seq_dev), 1)
    col_idx = lax.broadcasted_iota(jnp.int32, (1, seq_dev, seq_dev), 2)
    kq_prod = bdot(rows_cat(k_ref[0], q_ref[0]), k_ref[0], 2, 2)
    gram_buf[...] = kq_prod[:, :seq_dev]
    scores = jnp.where(row_idx >= col_idx, kq_prod[:, seq_dev:], 0.0)
    delta_buf[...] = dot_re(split(scores), do_ref[0], 1, 1)
    state_buf[...] = bdot(q_ref[0], do_ref[0], 1, 1)

    @pl.when(me < groups - 1)
    def _():
        hop(slot, step).wait_recv()

    @pl.when((me > 0) & (step >= SEND_SLOTS))
    def _():
        hop(slot, step).wait_send()
        front_hop(slot, step).wait_send()

    d_state = recv[from_next]
    d_delta = delta_buf[...] + dot_er(k_ref[0], split(d_state), 2, 1)
    d_rhs = dot_rr(split(t_ref[0]), split(d_delta), 1, 1)
    d_resid = beta3 * d_rhs
    rhs_buf[...] = d_rhs
    send[slot] = d_state + state_buf[...] - dot_er(k_ref[0], split(d_resid), 1, 1)
    dact[2] = d_resid.astype(BF16)

    d_out = do_ref[0]
    delta_split = split(d_ref[0])
    d_rhs = rhs_buf[...]
    by_delta = bdot(twice(rows_cat(d_out, *split(d_rhs)), 2), joined(delta_split, 2), 2, 2)

    @pl.when(me > 0)
    def _():
        hop(slot, step).start()

    d_scores = jnp.where(row_idx >= col_idx, by_delta[:, :seq_dev], 0.0).astype(BF16)
    d_low = jnp.where(row_idx > col_idx, -(by_delta[:, seq_dev:2 * seq_dev] + by_delta[:, 2 * seq_dev:]), 0.0)
    d_beta = jnp.sum(d_rhs * r_ref[0], axis=-1, keepdims=True) + jnp.sum(d_low * gram_buf[...], axis=-1, keepdims=True)
    d_gram = (beta3 * d_low).astype(BF16)
    by_state = bdot(twice(rows_cat(d_out, *split(beta3 * d_rhs)), 2), joined(split(s_ref[0]), 2), 2, 2)
    k_all = k_ref[0]
    by_key = bdot(rows_cat(d_scores, d_gram), k_all, 2, 1)
    dact[0] = (by_state[:, :seq_dev] + by_key[:, :seq_dev]).astype(BF16)
    d_key = by_key[:, seq_dev:] + bdot(rows_cat(d_gram, d_scores), rows_cat(k_all, q_ref[0]), 1, 1)
    d_key = d_key + dot_rr(delta_split, split(recv[from_next]), 2, 2) - (by_state[:, seq_dev:2 * seq_dev] + by_state[:, 2 * seq_dev:])
    dact[1] = d_key.astype(BF16)
    lane_idx = lax.broadcasted_iota(jnp.int32, (seq_dev, n_heads), 1)
    beta_grad = jnp.zeros((seq_dev, n_heads), F32)
    for head in range(n_heads):
        beta_grad = beta_grad + jnp.where(lane_idx == head, d_beta[head], 0.0)
    dlogit_ref[0] = (beta_grad.astype(BF16).astype(F32) * sig_beta * (1.0 - sig_beta)).astype(BF16)

    def act_head(head, carry):
        cols = head_cols(head)
        fill_ext(ext, (pq_ref, pk_ref, pv_ref), tail_ref, cols, head, model_dim)
        for branch in range(3):
            conv_sum = conv_rows(ext, branch, cols, taps_ref[branch, :, cols], seq_dev)
            sig = jax.nn.sigmoid(conv_sum)
            d_act = dact[branch, head].astype(F32)
            if branch < 2:
                act = conv_sum * sig
                inv_norm = lax.rsqrt(jnp.sum(act * act, axis=-1, keepdims=True) + 1e-6)
                unit = act * inv_norm
                d_act = inv_norm * (d_act - unit * jnp.sum(unit * d_act, axis=-1, keepdims=True))
            d_conv = d_act * (sig * (1.0 + conv_sum * (1.0 - sig)))
            dext[branch, pl.ds(0, seq_dev), cols] = d_conv
            front_send[slot, branch, :, cols] = d_conv[0:8]
            for tap_idx in range(CONV_TAPS):
                prod = d_conv * ext[branch, pl.ds(8 - PAD + tap_idx, seq_dev), cols]
                dtaps_ref[branch, tap_idx, :, cols] += jnp.sum(prod.reshape(seq_dev // 8, 8, HEAD_DIM), axis=0)
        return carry

    lax.fori_loop(0, n_heads, act_head, 0)

    @pl.when(me > 0)
    def _():
        front_hop(slot, step).start()

    @pl.when(me < groups - 1)
    def _():
        front_hop(slot, step).wait_recv()

    def conv_head(head, carry):
        cols = head_cols(head)
        for branch in range(3):
            taps = taps_ref[branch, :, cols]
            dext[branch, pl.ds(seq_dev, 8), cols] = front[from_next, branch, :, cols]
            total = dext[branch, pl.ds(PAD, seq_dev), cols] * taps[0:1]
            for tap_idx in range(1, CONV_TAPS):
                total = total + dext[branch, pl.ds(PAD - tap_idx, seq_dev), cols] * taps[tap_idx:tap_idx + 1]
            (dpq_ref, dpk_ref, dpv_ref)[branch][0, :, cols] = total.astype(BF16)
        return carry

    lax.fori_loop(0, n_heads, conv_head, 0)

    @pl.when((me > 0) & (step == n_steps - 1))
    def _():
        for back in range(min(SEND_SLOTS, recv.shape[0])):
            last = recv.shape[0] - 1 - back
            hop(last % SEND_SLOTS, last).wait_send()
            front_hop(last % SEND_SLOTS, last).wait_send()


def seq_block(shape):
    return pl.BlockSpec((1,) + tuple(shape[1:]), lambda step: (step,) + (0,) * (len(shape) - 1))


def whole_block(shape):
    return pl.BlockSpec(tuple(shape), lambda step: (0,) * len(shape))


def run_forward(groups, projs, tails, taps, logits, gate_pre, d_hidden, norm_f):
    n_seqs, seq_dev, model_dim = gate_pre.shape
    n_heads = model_dim // HEAD_DIM
    tok = jax.ShapeDtypeStruct((n_seqs, seq_dev, model_dim), BF16)
    per_head_b = jax.ShapeDtypeStruct((n_seqs, n_heads, seq_dev, HEAD_DIM), BF16)
    per_head_f = jax.ShapeDtypeStruct((n_seqs, n_heads, seq_dev, HEAD_DIM), F32)
    outs = [tok, tok, per_head_b, per_head_b, per_head_b,
            jax.ShapeDtypeStruct((n_seqs, n_heads, seq_dev, seq_dev), F32),
            jax.ShapeDtypeStruct((n_seqs, n_heads, HEAD_DIM, HEAD_DIM), F32),
            per_head_f, per_head_f, jax.ShapeDtypeStruct((8, HEAD_DIM), F32)]
    ins = [*projs, tails, taps, logits, gate_pre, d_hidden, norm_f]
    return pl.pallas_call(
        functools.partial(forward_kernel, groups),
        grid=(n_seqs,),
        out_shape=outs,
        in_specs=[seq_block(arr.shape) for arr in ins[:4]] + [whole_block(taps.shape)] + [seq_block(arr.shape) for arr in ins[5:8]] + [whole_block(norm_f.shape)],
        out_specs=[seq_block(out.shape) for out in outs[:-1]] + [whole_block(outs[-1].shape)],
        scratch_shapes=[
            pltpu.VMEM((n_seqs, n_heads, HEAD_DIM, HEAD_DIM), F32),
            pltpu.VMEM((SEND_SLOTS, n_heads, HEAD_DIM, HEAD_DIM), F32),
            pltpu.VMEM((3, seq_dev + 8, model_dim), F32),
            pltpu.VMEM((n_heads, seq_dev, HEAD_DIM), BF16),
            pltpu.VMEM((n_heads, seq_dev, HEAD_DIM), F32),
            pltpu.VMEM((n_heads, seq_dev, seq_dev), F32),
            pltpu.SemaphoreType.DMA((SEND_SLOTS,)),
            pltpu.SemaphoreType.DMA((n_seqs,)),
        ],
        compiler_params=pltpu.CompilerParams(collective_id=0, has_side_effects=True, vmem_limit_bytes=VMEM_LIMIT, dimension_semantics=('arbitrary',)),
        cost_estimate=pl.CostEstimate(flops=200_000_000_000, bytes_accessed=120_000_000, transcendentals=0),
        name='delta_forward',
    )(*ins)


def run_backward(groups, projs, tails, taps, logits, d_attn, q_act, k_act, t_mat, s_mat, r_mat, d_mat):
    n_seqs, seq_dev, model_dim = projs[0].shape
    n_heads = model_dim // HEAD_DIM
    tok = jax.ShapeDtypeStruct((n_seqs, seq_dev, model_dim), BF16)
    outs = [tok, tok, tok, jax.ShapeDtypeStruct(logits.shape, BF16), jax.ShapeDtypeStruct((3, CONV_TAPS, 8, model_dim), F32)]
    ins = [*projs, tails, taps, logits, d_attn, q_act, k_act, t_mat, s_mat, r_mat, d_mat]
    return pl.pallas_call(
        functools.partial(backward_kernel, groups),
        grid=(n_seqs,),
        out_shape=outs,
        in_specs=[seq_block(arr.shape) for arr in ins[:4]] + [whole_block(taps.shape)] + [seq_block(arr.shape) for arr in ins[5:]],
        out_specs=[seq_block(out.shape) for out in outs[:-1]] + [whole_block(outs[-1].shape)],
        scratch_shapes=[
            pltpu.VMEM((n_seqs, n_heads, HEAD_DIM, HEAD_DIM), F32),
            pltpu.VMEM((SEND_SLOTS, n_heads, HEAD_DIM, HEAD_DIM), F32),
            pltpu.VMEM((n_seqs, 3, 8, model_dim), F32),
            pltpu.VMEM((SEND_SLOTS, 3, 8, model_dim), F32),
            pltpu.VMEM((3, seq_dev + 8, model_dim), F32),
            pltpu.VMEM((3, seq_dev + 8, model_dim), F32),
            pltpu.VMEM((3, n_heads, seq_dev, HEAD_DIM), BF16),
            pltpu.VMEM((n_heads, seq_dev, seq_dev), F32),
            pltpu.VMEM((n_heads, seq_dev, HEAD_DIM), F32),
            pltpu.VMEM((n_heads, HEAD_DIM, HEAD_DIM), F32),
            pltpu.VMEM((n_heads, seq_dev, HEAD_DIM), F32),
            pltpu.SemaphoreType.DMA((SEND_SLOTS,)),
            pltpu.SemaphoreType.DMA((n_seqs,)),
            pltpu.SemaphoreType.DMA((SEND_SLOTS,)),
            pltpu.SemaphoreType.DMA((n_seqs,)),
        ],
        compiler_params=pltpu.CompilerParams(collective_id=1, has_side_effects=True, vmem_limit_bytes=VMEM_LIMIT, dimension_semantics=('arbitrary',)),
        cost_estimate=pl.CostEstimate(flops=250_000_000_000, bytes_accessed=120_000_000, transcendentals=0),
        name='delta_backward',
    )(*ins)


def tail_kernel(n_seqs, *refs):
    parts, (h_ref, dg_ref, dq_ref, dk_ref, dv_ref, dl_ref), (wo_ref, wg_ref, wq_ref, wk_ref, wv_ref, wb_ref) = refs[:6], refs[6:12], refs[12:18]
    sums, (y_ref, dx_ref) = refs[18:24], refs[24:26]
    own, pair, outer, inner, load_sem, psend, precv, osend, orecv, isend, irecv, store_sem, csend, crecv = refs[26:]
    step = pl.program_id(0)
    n_chunks = own.shape[0] // CHUNK
    last_step = n_chunks + LAG_END
    me = lax.axis_index('sp')
    chip = me // 2
    core = lax.rem(me, 2)
    partner = me + 1 - 2 * core
    is_end = (chip == 0) | (chip == 3)
    is_mid = (chip == 1) | (chip == 2)
    outer_dev = lax.rem(me + 8 + 2 - 4 * lax.rem(chip, 2), 8)
    inner_dev = lax.rem(me + 8 - 2 + 4 * lax.rem(chip, 2), 8)
    group_len = parts[0].shape[0] // 2 // CHUNK

    def rows(idx):
        return pl.ds(pl.multiple_of(idx * CHUNK, CHUNK), CHUNK)

    def half(idx, which):
        size = parts[idx].shape[0] // 2
        return pl.ds(pl.multiple_of(which * size, CHUNK), size)

    def buf_rows(idx):
        return pl.ds(idx * group_len * CHUNK, parts[idx].shape[0] // 2)

    def remote(src, dst, send_sem, recv_sem, dev):
        return pltpu.make_async_remote_copy(src_ref=src, dst_ref=dst, send_sem=send_sem, recv_sem=recv_sem, device_id={'sp': dev}, device_id_type=MESH)

    def load_copy(idx):
        return pltpu.make_async_copy(parts[idx].at[half(idx, core)], own.at[buf_rows(idx)], load_sem.at[idx])

    def pair_copy(idx):
        return remote(parts[idx].at[half(idx, 1 - core)], pair.at[buf_rows(idx)], psend.at[idx], precv.at[idx], partner)

    def outer_copy(src, idx):
        return remote(src.at[rows(idx)], outer.at[rows(idx)], osend.at[idx], orecv.at[idx], outer_dev)

    def inner_copy(idx):
        return remote(own.at[rows(idx)], inner.at[rows(idx)], isend.at[idx], irecv.at[idx], inner_dev)

    def store_copy(src, idx):
        return pltpu.make_async_copy(src.at[buf_rows(idx)], sums[idx].at[half(idx, core)], store_sem.at[idx])

    def give_copy(src, idx):
        return remote(src.at[buf_rows(idx)], sums[idx].at[half(idx, core)], csend.at[idx], crecv.at[idx], partner)

    @pl.when(step == 0)
    def _():
        barrier = pltpu.get_barrier_semaphore()
        for other in range(1, 8):
            pl.semaphore_signal(barrier, inc=1, device_id={'sp': lax.rem(me + other, 8)}, device_id_type=MESH)
        pl.semaphore_wait(barrier, 7)
        for idx in range(len(parts)):
            load_copy(idx).start()
            pair_copy(idx).start()

    @pl.when(is_end & (step >= 1) & (step <= n_chunks))
    def _():
        outer_copy(own, step - 1).start()

    @pl.when(is_mid & (step >= LAG_JOIN + 1) & (step <= n_chunks + LAG_JOIN))
    def _():
        inner_copy(step - LAG_JOIN - 1).start()

    @pl.when(is_mid & (step >= LAG_TOTAL + 1) & (step <= n_chunks + LAG_TOTAL))
    def _():
        outer_copy(pair, step - LAG_TOTAL - 1).start()

    for idx in range(len(parts)):
        final = idx * group_len + parts[idx].shape[0] // 2 // CHUNK - 1

        @pl.when(is_mid & (step == final + LAG_TOTAL + 1))
        def _():
            store_copy(pair, idx).start()
            give_copy(pair, idx).start()

        @pl.when(step == idx * group_len)
        def _():
            load_copy(idx).wait()
            pair_copy(idx).wait_recv()

    @pl.when(step < n_seqs)
    def _():
        y_ref[0] = lax.dot_general(h_ref[0], wo_ref[...], (((1,), (0,)), ((), ())), preferred_element_type=F32).astype(BF16)
        total = lax.dot_general(dg_ref[0], wg_ref[...], (((1,), (1,)), ((), ())), preferred_element_type=F32)
        for grad_ref, w_ref in ((dl_ref, wb_ref), (dq_ref, wq_ref), (dk_ref, wk_ref), (dv_ref, wv_ref)):
            total = total + lax.dot_general(grad_ref[0], w_ref[...], (((1,), (1,)), ((), ())), preferred_element_type=F32)
        dx_ref[0] = total.astype(BF16)

    @pl.when(step < n_chunks)
    def _():
        own[rows(step)] = own[rows(step)] + pair[rows(step)]

    @pl.when(is_mid & (step >= LAG_JOIN) & (step < n_chunks + LAG_JOIN))
    def _():
        idx = step - LAG_JOIN
        outer_copy(pair, idx).wait_recv()
        own[rows(idx)] = own[rows(idx)] + outer[rows(idx)]

    @pl.when(is_mid & (step >= LAG_TOTAL) & (step < n_chunks + LAG_TOTAL))
    def _():
        idx = step - LAG_TOTAL
        inner_copy(idx).wait_recv()
        pair[rows(idx)] = own[rows(idx)] + inner[rows(idx)]

    @pl.when(is_end & (step >= LAG_END) & (step < n_chunks + LAG_END))
    def _():
        outer_copy(own, step - LAG_END).wait_recv()

    for idx in range(len(parts)):
        final = idx * group_len + parts[idx].shape[0] // 2 // CHUNK - 1

        @pl.when(is_end & (step == final + LAG_END))
        def _():
            store_copy(outer, idx).start()
            give_copy(outer, idx).start()

    @pl.when(step == last_step)
    def _():
        for idx in range(len(parts)):
            pair_copy(idx).wait_send()
            store_copy(outer, idx).wait()
            give_copy(outer, idx).wait()

        def drain_outer(idx, carry):
            outer_copy(own, idx).wait_send()
            return carry

        lax.fori_loop(0, n_chunks, drain_outer, 0)

        @pl.when(is_mid)
        def _():
            def drain_inner(idx, carry):
                inner_copy(idx).wait_send()
                return carry

            lax.fori_loop(0, n_chunks, drain_inner, 0)


def run_tail(parts, acts, weights):
    n_seqs, seq_dev, model_dim = acts[0].shape
    n_rows = sum(part.shape[0] for part in parts) // 2
    n_chunks = n_rows // CHUNK
    n_parts = len(parts)
    any_spec = pl.BlockSpec(memory_space=pl.ANY)

    def row_block(arr):
        return pl.BlockSpec((1,) + tuple(arr.shape[1:]), lambda step: (jnp.minimum(step, n_seqs - 1), 0, 0))

    outs = [jax.ShapeDtypeStruct(part.shape, F32) for part in parts] + [jax.ShapeDtypeStruct(acts[0].shape, BF16)] * 2
    buf = pltpu.VMEM((n_rows, model_dim), F32)
    part_sems = pltpu.SemaphoreType.DMA((n_parts,))
    chunk_sems = pltpu.SemaphoreType.DMA((n_chunks,))
    return pl.pallas_call(
        functools.partial(tail_kernel, n_seqs),
        grid=(n_chunks + LAG_END + 1,),
        out_shape=outs,
        in_specs=[any_spec] * n_parts + [row_block(arr) for arr in acts] + [pl.BlockSpec(memory_space=pltpu.VMEM) for _ in weights],
        out_specs=[any_spec] * n_parts + [row_block(acts[0])] * 2,
        scratch_shapes=[buf] * 4 + [part_sems] * 3 + [chunk_sems] * 4 + [part_sems] * 3,
        compiler_params=pltpu.CompilerParams(collective_id=2, has_side_effects=True, vmem_limit_bytes=62 * 1024 * 1024, dimension_semantics=('arbitrary',)),
        cost_estimate=pl.CostEstimate(flops=250_000_000_000, bytes_accessed=120_000_000, transcendentals=0),
        name='sum_and_project',
    )(*parts, *acts, *weights)


def solution(mesh):
    groups = mesh.shape['sp']
    to_next = [(source, source + 1) for source in range(groups - 1)]
    seq_spec = P('dp', 'sp', None)
    full_mat = P(None, None)
    part_mat = P('dp', None)

    def local_step(x_in, dy_out, w_query, w_key, w_value, w_beta, conv_query, conv_key, conv_value, w_gate, norm_weight, w_out):
        seq_dev = x_in.shape[1]
        projs = [project(x_in, weight).astype(BF16) for weight in (w_query, w_key, w_value)]
        tails = lax.ppermute(jnp.concatenate([proj[:, seq_dev - PAD:] for proj in projs], axis=-1), 'sp', to_next)
        taps = jnp.stack([conv_query, conv_key, conv_value]).astype(F32)
        logits = project(x_in, w_beta).astype(BF16)
        gate_pre = project(x_in, w_gate).astype(BF16)
        d_hidden = back_project(dy_out, w_out).astype(BF16)
        norm_f = norm_weight.astype(F32).reshape(1, HEAD_DIM)
        hidden, d_gate, d_attn, q_act, k_act, t_mat, s_mat, r_mat, d_mat, dnorm = run_forward(groups, projs, tails, taps, logits, gate_pre, d_hidden, norm_f)
        dp_q, dp_k, dp_v, d_logit, dtaps = run_backward(groups, projs, tails, taps, logits, d_attn, q_act, k_act, t_mat, s_mat, r_mat, d_mat)
        model_dim = x_in.shape[2]
        small = jnp.concatenate([
            jnp.einsum('bte,btd->ed', d_logit, x_in, preferred_element_type=F32),
            jnp.sum(dtaps, axis=2).reshape(3 * CONV_TAPS, model_dim),
            jnp.pad(jnp.sum(dnorm, axis=0, keepdims=True), ((0, 0), (0, model_dim - HEAD_DIM)))])
        n_heads = w_beta.shape[1]
        small = jnp.pad(small, ((0, 2 * CHUNK - small.shape[0]), (0, 0)))
        grads = (weight_grad(x_in, d_gate), weight_grad(hidden, dy_out), weight_grad(x_in, dp_q), weight_grad(x_in, dp_k), weight_grad(x_in, dp_v), small)
        dw_gate, dw_out, dw_q, dw_k, dw_v, small, y_out, dx_in = run_tail(
            grads, (hidden, d_gate, dp_q, dp_k, dp_v, d_logit), (w_out, w_gate, w_query, w_key, w_value, w_beta))
        dtaps = small[n_heads:n_heads + 3 * CONV_TAPS].reshape(3, CONV_TAPS, model_dim)
        dnorm = small[n_heads + 3 * CONV_TAPS, :HEAD_DIM]
        return (y_out, dx_in, dw_q, dw_k, dw_v, small[:n_heads].T, dtaps[0], dtaps[1], dtaps[2], dw_gate, dnorm, dw_out)

    in_specs = (seq_spec, seq_spec) + (full_mat,) * 8 + (P(None), full_mat)
    out_specs = (seq_spec, seq_spec) + (part_mat,) * 8 + (P('dp'), part_mat)
    return jax.shard_map(local_step, mesh=mesh, in_specs=in_specs, out_specs=out_specs, check_vma=False)
```

```python
import functools
import jax
import jax.numpy as jnp
from jax import lax
from jax.experimental import pallas as pl
from jax.experimental.pallas import tpu as pltpu
from jax.sharding import PartitionSpec as P

HEAD_DIM = 128
CONV_TAPS = 4
PAD = CONV_TAPS - 1
SEND_SLOTS = 4
CHUNK = 32
LAG_JOIN = 3
LAG_TOTAL = 7
LAG_END = 12
DENSE_EVERY = 2
F32 = jnp.float32
BF16 = jnp.bfloat16
MESH = pl.DeviceIdType.MESH
VMEM_LIMIT = 60 * 1024 * 1024


def project(act_in, weight):
    return jnp.einsum('btd,de->bte', act_in, weight, preferred_element_type=F32)


def back_project(grad_in, weight):
    return jnp.einsum('bte,de->btd', grad_in, weight, preferred_element_type=F32)


def weight_grad(act_in, grad_in):
    return jnp.einsum('btd,bte->de', act_in, grad_in, preferred_element_type=F32)


def bdot(lhs, rhs, lhs_dim, rhs_dim):
    return lax.dot_general(lhs, rhs, (((lhs_dim,), (rhs_dim,)), ((0,), (0,))), preferred_element_type=F32)


def split(value):
    high = value.astype(BF16)
    return high, (value - high.astype(F32)).astype(BF16)


def rows_cat(*parts):
    return jnp.concatenate(parts, axis=1)


def twice(value, axis):
    return jnp.concatenate([value, value], axis=axis)


def joined(pair, axis):
    return jnp.concatenate(pair, axis=axis)


def dot_er(lhs, rhs, lhs_dim, rhs_dim):
    if lhs_dim == 2 and lhs.shape[2] == HEAD_DIM:
        return bdot(twice(lhs, 2), joined(rhs, rhs_dim), 2, rhs_dim)
    return bdot(lhs, rhs[0], lhs_dim, rhs_dim) + bdot(lhs, rhs[1], lhs_dim, rhs_dim)


def dot_re(lhs, rhs, lhs_dim, rhs_dim):
    return bdot(lhs[0], rhs, lhs_dim, rhs_dim) + bdot(lhs[1], rhs, lhs_dim, rhs_dim)


def dot_rr(lhs, rhs, lhs_dim, rhs_dim):
    if lhs_dim == 2:
        n_rows = lhs[0].shape[1]
        both = rows_cat(*lhs)
        if both.shape[2] == HEAD_DIM:
            prod = bdot(twice(both, 2), joined(rhs, rhs_dim), 2, rhs_dim)
            return prod[:, :n_rows] + prod[:, n_rows:]
        prod = bdot(both, rhs[0], 2, rhs_dim)
        return prod[:, :n_rows] + (prod[:, n_rows:] + bdot(lhs[0], rhs[1], 2, rhs_dim))
    return bdot(lhs[0], rhs[0], lhs_dim, rhs_dim) + (bdot(lhs[0], rhs[1], lhs_dim, rhs_dim) + bdot(lhs[1], rhs[0], lhs_dim, rhs_dim))


def block_inverse(low_mat, row_idx, col_idx):
    size = low_mat.shape[-1]
    eye = (row_idx == col_idx).astype(F32)
    low_split = split(low_mat)
    inv = eye - jnp.where(row_idx // 2 == col_idx // 2, low_mat, 0.0)
    width = 2
    while width < size:
        fresh = (row_idx // (2 * width) == col_idx // (2 * width)) & (row_idx // width != col_idx // width)
        corner = jnp.where(fresh, low_mat, 0.0).astype(BF16)
        inv_b = inv.astype(BF16)
        inv = inv - bdot(bdot(inv_b, corner, 2, 1).astype(BF16), inv_b, 2, 1)
        width *= 2
    inv_split = split(inv)
    resid = eye - inv - dot_rr(low_split, inv_split, 2, 1)
    return inv + bdot(inv_split[0], resid.astype(BF16), 2, 1)


def head_cols(head):
    return pl.ds(pl.multiple_of(head * HEAD_DIM, HEAD_DIM), HEAD_DIM)


def front_lanes(branch, row):
    return pl.ds((branch * PAD + row) * HEAD_DIM, HEAD_DIM)


def head_columns(array_in, n_heads):
    return jnp.concatenate([array_in[:, head:head + 1][None] for head in range(n_heads)], axis=0)


def entry_barrier(me, groups):
    barrier = pltpu.get_barrier_semaphore()
    for step in (1, groups - 1):
        pl.semaphore_signal(barrier, inc=1, device_id={'sp': lax.rem(me + step, groups)}, device_id_type=MESH)
    pl.semaphore_wait(barrier, 2)


def conv_rows(ext_ref, branch, cols, taps, seq_dev):
    total = ext_ref[branch, pl.ds(8 - PAD, seq_dev), cols] * taps[0:1]
    for tap_idx in range(1, CONV_TAPS):
        total = total + ext_ref[branch, pl.ds(8 - PAD + tap_idx, seq_dev), cols] * taps[tap_idx:tap_idx + 1]
    return total


def fill_ext(ext_ref, p_refs, tail_ref, cols, head, model_dim):
    seq_dev = p_refs[0].shape[1]
    for branch in range(3):
        tail_cols = pl.ds(pl.multiple_of(branch * model_dim + head * HEAD_DIM, HEAD_DIM), HEAD_DIM)
        ext_ref[branch, pl.ds(8 - PAD, PAD), cols] = tail_ref[0, :, tail_cols].astype(F32)
        ext_ref[branch, pl.ds(8, seq_dev), cols] = p_refs[branch][0, :, cols].astype(F32)


def forward_kernel(groups, pq_ref, pk_ref, pv_ref, tail_ref, taps_ref, logit_ref, z_ref, dh_ref, norm_ref,
                   h_ref, dz_ref, do_ref, q_ref, k_ref, t_ref, s_ref, r_ref, d_ref, dnorm_ref,
                   recv, send, ext, v_buf, o_buf, score_buf, send_sem, recv_sem):
    step = pl.program_id(0)
    n_steps = pl.num_programs(0)
    me = lax.axis_index('sp')
    seq_dev = pq_ref.shape[1]
    model_dim = pq_ref.shape[2]
    n_heads = model_dim // HEAD_DIM
    slot = lax.rem(step, SEND_SLOTS)

    def hop(slot_idx, step_idx):
        return pltpu.make_async_remote_copy(
            src_ref=send.at[slot_idx], dst_ref=recv.at[step_idx], send_sem=send_sem.at[slot_idx], recv_sem=recv_sem.at[step_idx],
            device_id={'sp': lax.rem(me + 1, groups)}, device_id_type=MESH)

    @pl.when(step == 0)
    def _():
        entry_barrier(me, groups)
        dnorm_ref[...] = jnp.zeros_like(dnorm_ref)

        @pl.when(me == 0)
        def _():
            recv[0] = jnp.zeros(recv.shape[1:], F32)

    def act_head(head, carry):
        cols = head_cols(head)
        fill_ext(ext, (pq_ref, pk_ref, pv_ref), tail_ref, cols, head, model_dim)
        for branch in range(3):
            act = jax.nn.silu(conv_rows(ext, branch, cols, taps_ref[branch, :, cols], seq_dev))
            if branch < 2:
                act = act * lax.rsqrt(jnp.sum(act * act, axis=-1, keepdims=True) + 1e-6)
                (q_ref, k_ref)[branch][0, head] = act.astype(BF16)
            else:
                v_buf[head] = act.astype(BF16)
        return carry

    lax.fori_loop(0, n_heads, act_head, 0)

    beta = jax.nn.sigmoid(logit_ref[0].astype(F32)).astype(BF16).astype(F32)
    beta3 = head_columns(beta, n_heads)
    q_all = q_ref[0]
    k_all = k_ref[0]
    row_idx = lax.broadcasted_iota(jnp.int32, (1, seq_dev, seq_dev), 1)
    col_idx = lax.broadcasted_iota(jnp.int32, (1, seq_dev, seq_dev), 2)
    kq_all = rows_cat(k_all, q_all)
    kq_prod = bdot(kq_all, k_all, 2, 2)
    gram = kq_prod[:, :seq_dev]
    score_buf[...] = jnp.where(row_idx >= col_idx, kq_prod[:, seq_dev:], 0.0)
    t_ref[0] = block_inverse(jnp.where(row_idx > col_idx, beta3 * gram, 0.0), row_idx, col_idx)

    @pl.when(me > 0)
    def _():
        hop(slot, step).wait_recv()

    @pl.when((me < groups - 1) & (step >= SEND_SLOTS))
    def _():
        hop(slot, step).wait_send()

    state = recv[step * jnp.minimum(me, 1)]
    s_ref[0] = state
    kq_state = dot_er(rows_cat(k_ref[0], q_ref[0]), split(state), 2, 1)
    resid = v_buf[...].astype(F32) - kq_state[:, :seq_dev]
    r_ref[0] = resid
    delta = dot_rr(split(t_ref[0]), split(beta3 * resid), 2, 1)
    d_ref[0] = delta
    delta_split = split(delta)
    send[slot] = state + dot_er(k_ref[0], delta_split, 1, 1)
    o_buf[...] = (kq_state[:, seq_dev:] + dot_rr(split(score_buf[...]), delta_split, 2, 1)).astype(BF16).astype(F32)

    @pl.when(me < groups - 1)
    def _():
        hop(slot, step).start()

    def post_head(head, carry):
        cols = head_cols(head)
        attn = o_buf[head]
        norm_w = norm_ref[...]
        z_in = z_ref[0, :, cols].astype(F32)
        dh_in = dh_ref[0, :, cols].astype(F32)
        inv_rms = lax.rsqrt(jnp.mean(attn * attn, axis=-1, keepdims=True) + 1e-5)
        unit = attn * inv_rms
        normed = unit * norm_w
        sig = jax.nn.sigmoid(z_in)
        gate = z_in * sig
        h_ref[0, :, cols] = (normed * gate).astype(BF16)
        d_normed = dh_in * gate
        dz_ref[0, :, cols] = (dh_in * normed * (sig * (1.0 + z_in * (1.0 - sig)))).astype(BF16)
        d_unit = d_normed * norm_w
        dnorm_ref[...] += jnp.sum((d_normed * unit).reshape(seq_dev // 8, 8, HEAD_DIM), axis=0)
        do_ref[0, head] = (inv_rms * (d_unit - unit * jnp.mean(unit * d_unit, axis=-1, keepdims=True))).astype(BF16)
        return carry

    lax.fori_loop(0, n_heads, post_head, 0)

    @pl.when((me < groups - 1) & (step == n_steps - 1))
    def _():
        for back in range(min(SEND_SLOTS, recv.shape[0])):
            last = recv.shape[0] - 1 - back
            hop(last % SEND_SLOTS, last).wait_send()


def backward_kernel(groups, pq_ref, pk_ref, pv_ref, tail_ref, taps_ref, logit_ref, do_ref, q_ref, k_ref, t_ref, s_ref, r_ref, d_ref,
                    dpq_ref, dpk_ref, dpv_ref, dlogit_ref, dtaps_ref,
                    recv, send, front, front_send, ext, dext, dact, gram_buf, delta_buf, state_buf, rhs_buf, send_sem, recv_sem, fsend_sem, frecv_sem):
    step = pl.program_id(0)
    n_steps = pl.num_programs(0)
    me = lax.axis_index('sp')
    seq_dev = pq_ref.shape[1]
    model_dim = pq_ref.shape[2]
    n_heads = model_dim // HEAD_DIM
    slot = lax.rem(step, SEND_SLOTS)
    to_prev = lax.rem(me + groups - 1, groups)

    def hop(slot_idx, step_idx):
        return pltpu.make_async_remote_copy(
            src_ref=send.at[slot_idx], dst_ref=recv.at[step_idx], send_sem=send_sem.at[slot_idx], recv_sem=recv_sem.at[step_idx],
            device_id={'sp': to_prev}, device_id_type=MESH)

    def front_hop(slot_idx, step_idx):
        return pltpu.make_async_remote_copy(
            src_ref=front_send.at[slot_idx], dst_ref=front.at[step_idx], send_sem=fsend_sem.at[slot_idx], recv_sem=frecv_sem.at[step_idx],
            device_id={'sp': to_prev}, device_id_type=MESH)

    @pl.when(step == 0)
    def _():
        entry_barrier(me, groups)
        dtaps_ref[...] = jnp.zeros_like(dtaps_ref)

        @pl.when(me == groups - 1)
        def _():
            recv[0] = jnp.zeros(recv.shape[1:], F32)
            front[0] = jnp.zeros(front.shape[1:], F32)

    sig_beta = jax.nn.sigmoid(logit_ref[0].astype(F32))
    beta3 = head_columns(sig_beta.astype(BF16).astype(F32), n_heads)
    from_next = step * jnp.minimum(groups - 1 - me, 1)
    row_idx = lax.broadcasted_iota(jnp.int32, (1, seq_dev, seq_dev), 1)
    col_idx = lax.broadcasted_iota(jnp.int32, (1, seq_dev, seq_dev), 2)
    kq_prod = bdot(rows_cat(k_ref[0], q_ref[0]), k_ref[0], 2, 2)
    gram_buf[...] = kq_prod[:, :seq_dev]
    scores = jnp.where(row_idx >= col_idx, kq_prod[:, seq_dev:], 0.0)
    delta_buf[...] = dot_re(split(scores), do_ref[0], 1, 1)
    state_buf[...] = bdot(q_ref[0], do_ref[0], 1, 1)

    @pl.when(me < groups - 1)
    def _():
        hop(slot, step).wait_recv()

    @pl.when((me > 0) & (step >= SEND_SLOTS))
    def _():
        hop(slot, step).wait_send()
        front_hop(slot, step).wait_send()

    d_state = recv[from_next]
    d_delta = delta_buf[...] + dot_er(k_ref[0], split(d_state), 2, 1)
    d_rhs = dot_rr(split(t_ref[0]), split(d_delta), 1, 1)
    d_resid = beta3 * d_rhs
    rhs_buf[...] = d_rhs
    send[slot] = d_state + state_buf[...] - dot_er(k_ref[0], split(d_resid), 1, 1)
    dact[2] = d_resid.astype(BF16)

    d_out = do_ref[0]
    delta_split = split(d_ref[0])
    d_rhs = rhs_buf[...]
    by_delta = bdot(twice(rows_cat(d_out, *split(d_rhs)), 2), joined(delta_split, 2), 2, 2)

    @pl.when(me > 0)
    def _():
        hop(slot, step).start()

    d_scores = jnp.where(row_idx >= col_idx, by_delta[:, :seq_dev], 0.0).astype(BF16)
    d_low = jnp.where(row_idx > col_idx, -(by_delta[:, seq_dev:2 * seq_dev] + by_delta[:, 2 * seq_dev:]), 0.0)
    d_beta = jnp.sum(d_rhs * r_ref[0], axis=-1, keepdims=True) + jnp.sum(d_low * gram_buf[...], axis=-1, keepdims=True)
    d_gram = (beta3 * d_low).astype(BF16)
    by_state = bdot(twice(rows_cat(d_out, *split(beta3 * d_rhs)), 2), joined(split(s_ref[0]), 2), 2, 2)
    k_all = k_ref[0]
    by_key = bdot(rows_cat(d_scores, d_gram), k_all, 2, 1)
    dact[0] = (by_state[:, :seq_dev] + by_key[:, :seq_dev]).astype(BF16)
    d_key = by_key[:, seq_dev:] + bdot(rows_cat(d_gram, d_scores), rows_cat(k_all, q_ref[0]), 1, 1)
    d_key = d_key + dot_rr(delta_split, split(recv[from_next]), 2, 2) - (by_state[:, seq_dev:2 * seq_dev] + by_state[:, 2 * seq_dev:])
    dact[1] = d_key.astype(BF16)
    lane_idx = lax.broadcasted_iota(jnp.int32, (seq_dev, n_heads), 1)
    beta_grad = jnp.zeros((seq_dev, n_heads), F32)
    for head in range(n_heads):
        beta_grad = beta_grad + jnp.where(lane_idx == head, d_beta[head], 0.0)
    dlogit_ref[0] = (beta_grad.astype(BF16).astype(F32) * sig_beta * (1.0 - sig_beta)).astype(BF16)

    def act_head(head, carry):
        cols = head_cols(head)
        fill_ext(ext, (pq_ref, pk_ref, pv_ref), tail_ref, cols, head, model_dim)
        for branch in range(3):
            conv_sum = conv_rows(ext, branch, cols, taps_ref[branch, :, cols], seq_dev)
            sig = jax.nn.sigmoid(conv_sum)
            d_act = dact[branch, head].astype(F32)
            if branch < 2:
                act = conv_sum * sig
                inv_norm = lax.rsqrt(jnp.sum(act * act, axis=-1, keepdims=True) + 1e-6)
                unit = act * inv_norm
                d_act = inv_norm * (d_act - unit * jnp.sum(unit * d_act, axis=-1, keepdims=True))
            d_conv = d_act * (sig * (1.0 + conv_sum * (1.0 - sig)))
            dext[branch, pl.ds(0, seq_dev), cols] = d_conv
            for tap_idx in range(CONV_TAPS):
                prod = d_conv * ext[branch, pl.ds(8 - PAD + tap_idx, seq_dev), cols]
                dtaps_ref[branch, tap_idx, :, cols] += jnp.sum(prod.reshape(seq_dev // 8, 8, HEAD_DIM), axis=0)
        return carry

    lax.fori_loop(0, n_heads, act_head, 0)

    for branch in range(3):
        for row in range(PAD):
            for head in range(n_heads):
                front_send[slot, head:head + 1, front_lanes(branch, row)] = dext[branch, row:row + 1, head * HEAD_DIM:(head + 1) * HEAD_DIM]

    @pl.when(me < groups - 1)
    def _():
        front_hop(slot, step).wait_recv()

    for branch in range(3):
        for row in range(PAD):
            for head in range(n_heads):
                dext[branch, seq_dev + row:seq_dev + row + 1, head * HEAD_DIM:(head + 1) * HEAD_DIM] = front[from_next, head:head + 1, front_lanes(branch, row)]

    @pl.when(me > 0)
    def _():
        front_hop(slot, step).start()

    def conv_head(head, carry):
        cols = head_cols(head)
        for branch in range(3):
            taps = taps_ref[branch, :, cols]
            total = dext[branch, pl.ds(PAD, seq_dev), cols] * taps[0:1]
            for tap_idx in range(1, CONV_TAPS):
                total = total + dext[branch, pl.ds(PAD - tap_idx, seq_dev), cols] * taps[tap_idx:tap_idx + 1]
            (dpq_ref, dpk_ref, dpv_ref)[branch][0, :, cols] = total.astype(BF16)
        return carry

    lax.fori_loop(0, n_heads, conv_head, 0)

    @pl.when((me > 0) & (step == n_steps - 1))
    def _():
        for back in range(min(SEND_SLOTS, recv.shape[0])):
            last = recv.shape[0] - 1 - back
            hop(last % SEND_SLOTS, last).wait_send()
            front_hop(last % SEND_SLOTS, last).wait_send()


def seq_block(shape):
    return pl.BlockSpec((1,) + tuple(shape[1:]), lambda step: (step,) + (0,) * (len(shape) - 1))


def whole_block(shape):
    return pl.BlockSpec(tuple(shape), lambda step: (0,) * len(shape))


def run_forward(groups, projs, tails, taps, logits, gate_pre, d_hidden, norm_f):
    n_seqs, seq_dev, model_dim = gate_pre.shape
    n_heads = model_dim // HEAD_DIM
    tok = jax.ShapeDtypeStruct((n_seqs, seq_dev, model_dim), BF16)
    per_head_b = jax.ShapeDtypeStruct((n_seqs, n_heads, seq_dev, HEAD_DIM), BF16)
    per_head_f = jax.ShapeDtypeStruct((n_seqs, n_heads, seq_dev, HEAD_DIM), F32)
    outs = [tok, tok, per_head_b, per_head_b, per_head_b,
            jax.ShapeDtypeStruct((n_seqs, n_heads, seq_dev, seq_dev), F32),
            jax.ShapeDtypeStruct((n_seqs, n_heads, HEAD_DIM, HEAD_DIM), F32),
            per_head_f, per_head_f, jax.ShapeDtypeStruct((8, HEAD_DIM), F32)]
    ins = [*projs, tails, taps, logits, gate_pre, d_hidden, norm_f]
    return pl.pallas_call(
        functools.partial(forward_kernel, groups),
        grid=(n_seqs,),
        out_shape=outs,
        in_specs=[seq_block(arr.shape) for arr in ins[:4]] + [whole_block(taps.shape)] + [seq_block(arr.shape) for arr in ins[5:8]] + [whole_block(norm_f.shape)],
        out_specs=[seq_block(out.shape) for out in outs[:-1]] + [whole_block(outs[-1].shape)],
        scratch_shapes=[
            pltpu.VMEM((n_seqs, n_heads, HEAD_DIM, HEAD_DIM), F32),
            pltpu.VMEM((SEND_SLOTS, n_heads, HEAD_DIM, HEAD_DIM), F32),
            pltpu.VMEM((3, seq_dev + 8, model_dim), F32),
            pltpu.VMEM((n_heads, seq_dev, HEAD_DIM), BF16),
            pltpu.VMEM((n_heads, seq_dev, HEAD_DIM), F32),
            pltpu.VMEM((n_heads, seq_dev, seq_dev), F32),
            pltpu.SemaphoreType.DMA((SEND_SLOTS,)),
            pltpu.SemaphoreType.DMA((n_seqs,)),
        ],
        compiler_params=pltpu.CompilerParams(collective_id=0, has_side_effects=True, vmem_limit_bytes=VMEM_LIMIT, dimension_semantics=('arbitrary',)),
        cost_estimate=pl.CostEstimate(flops=200_000_000_000, bytes_accessed=120_000_000, transcendentals=0),
        name='delta_forward',
    )(*ins)


def run_backward(groups, projs, tails, taps, logits, d_attn, q_act, k_act, t_mat, s_mat, r_mat, d_mat):
    n_seqs, seq_dev, model_dim = projs[0].shape
    n_heads = model_dim // HEAD_DIM
    tok = jax.ShapeDtypeStruct((n_seqs, seq_dev, model_dim), BF16)
    outs = [tok, tok, tok, jax.ShapeDtypeStruct(logits.shape, BF16), jax.ShapeDtypeStruct((3, CONV_TAPS, 8, model_dim), F32)]
    ins = [*projs, tails, taps, logits, d_attn, q_act, k_act, t_mat, s_mat, r_mat, d_mat]
    return pl.pallas_call(
        functools.partial(backward_kernel, groups),
        grid=(n_seqs,),
        out_shape=outs,
        in_specs=[seq_block(arr.shape) for arr in ins[:4]] + [whole_block(taps.shape)] + [seq_block(arr.shape) for arr in ins[5:]],
        out_specs=[seq_block(out.shape) for out in outs[:-1]] + [whole_block(outs[-1].shape)],
        scratch_shapes=[
            pltpu.VMEM((n_seqs, n_heads, HEAD_DIM, HEAD_DIM), F32),
            pltpu.VMEM((SEND_SLOTS, n_heads, HEAD_DIM, HEAD_DIM), F32),
            pltpu.VMEM((n_seqs, n_heads, 3 * PAD * HEAD_DIM), F32),
            pltpu.VMEM((SEND_SLOTS, n_heads, 3 * PAD * HEAD_DIM), F32),
            pltpu.VMEM((3, seq_dev + 8, model_dim), F32),
            pltpu.VMEM((3, seq_dev + 8, model_dim), F32),
            pltpu.VMEM((3, n_heads, seq_dev, HEAD_DIM), BF16),
            pltpu.VMEM((n_heads, seq_dev, seq_dev), F32),
            pltpu.VMEM((n_heads, seq_dev, HEAD_DIM), F32),
            pltpu.VMEM((n_heads, HEAD_DIM, HEAD_DIM), F32),
            pltpu.VMEM((n_heads, seq_dev, HEAD_DIM), F32),
            pltpu.SemaphoreType.DMA((SEND_SLOTS,)),
            pltpu.SemaphoreType.DMA((n_seqs,)),
            pltpu.SemaphoreType.DMA((SEND_SLOTS,)),
            pltpu.SemaphoreType.DMA((n_seqs,)),
        ],
        compiler_params=pltpu.CompilerParams(collective_id=1, has_side_effects=True, vmem_limit_bytes=VMEM_LIMIT, dimension_semantics=('arbitrary',)),
        cost_estimate=pl.CostEstimate(flops=250_000_000_000, bytes_accessed=120_000_000, transcendentals=0),
        name='delta_backward',
    )(*ins)


def tail_kernel(n_seqs, *refs):
    parts, (h_ref, dg_ref, dq_ref, dk_ref, dv_ref, dl_ref), (wo_ref, wg_ref, wq_ref, wk_ref, wv_ref, wb_ref) = refs[:6], refs[6:12], refs[12:18]
    sums, (y_ref, dx_ref) = refs[18:24], refs[24:26]
    own, pair, outer, inner, load_sem, psend, precv, osend, orecv, isend, irecv, store_sem, csend, crecv = refs[26:]
    step = pl.program_id(0)
    n_chunks = own.shape[0] // CHUNK
    last_step = n_chunks + LAG_END
    me = lax.axis_index('sp')
    chip = me // 2
    core = lax.rem(me, 2)
    partner = me + 1 - 2 * core
    is_end = (chip == 0) | (chip == 3)
    is_mid = (chip == 1) | (chip == 2)
    outer_dev = lax.rem(me + 8 + 2 - 4 * lax.rem(chip, 2), 8)
    inner_dev = lax.rem(me + 8 - 2 + 4 * lax.rem(chip, 2), 8)
    group_len = parts[0].shape[0] // 2 // CHUNK

    def rows(idx):
        return pl.ds(pl.multiple_of(idx * CHUNK, CHUNK), CHUNK)

    def half(idx, which):
        size = parts[idx].shape[0] // 2
        return pl.ds(pl.multiple_of(which * size, CHUNK), size)

    def buf_rows(idx):
        return pl.ds(idx * group_len * CHUNK, parts[idx].shape[0] // 2)

    def remote(src, dst, send_sem, recv_sem, dev):
        return pltpu.make_async_remote_copy(src_ref=src, dst_ref=dst, send_sem=send_sem, recv_sem=recv_sem, device_id={'sp': dev}, device_id_type=MESH)

    def load_copy(idx):
        return pltpu.make_async_copy(parts[idx].at[half(idx, core)], own.at[buf_rows(idx)], load_sem.at[idx])

    def pair_copy(idx):
        return remote(parts[idx].at[half(idx, 1 - core)], pair.at[buf_rows(idx)], psend.at[idx], precv.at[idx], partner)

    def outer_copy(src, idx):
        return remote(src.at[rows(idx)], outer.at[rows(idx)], osend.at[idx], orecv.at[idx], outer_dev)

    def inner_copy(idx):
        return remote(own.at[rows(idx)], inner.at[rows(idx)], isend.at[idx], irecv.at[idx], inner_dev)

    def store_copy(src, idx):
        return pltpu.make_async_copy(src.at[buf_rows(idx)], sums[idx].at[half(idx, core)], store_sem.at[idx])

    def give_copy(src, idx):
        return remote(src.at[buf_rows(idx)], sums[idx].at[half(idx, core)], csend.at[idx], crecv.at[idx], partner)

    @pl.when(step == 0)
    def _():
        barrier = pltpu.get_barrier_semaphore()
        for other in range(1, 8):
            pl.semaphore_signal(barrier, inc=1, device_id={'sp': lax.rem(me + other, 8)}, device_id_type=MESH)
        pl.semaphore_wait(barrier, 7)
        for idx in range(len(parts)):
            load_copy(idx).start()
            pair_copy(idx).start()

    @pl.when(is_end & (step >= 1) & (step <= n_chunks))
    def _():
        outer_copy(own, step - 1).start()

    @pl.when(is_mid & (step >= LAG_JOIN + 1) & (step <= n_chunks + LAG_JOIN))
    def _():
        inner_copy(step - LAG_JOIN - 1).start()

    @pl.when(is_mid & (step >= LAG_TOTAL + 1) & (step <= n_chunks + LAG_TOTAL))
    def _():
        outer_copy(pair, step - LAG_TOTAL - 1).start()

    for idx in range(len(parts)):
        final = idx * group_len + parts[idx].shape[0] // 2 // CHUNK - 1

        @pl.when(is_mid & (step == final + LAG_TOTAL + 1))
        def _():
            store_copy(pair, idx).start()
            give_copy(pair, idx).start()

        @pl.when(step == idx * group_len)
        def _():
            load_copy(idx).wait()
            pair_copy(idx).wait_recv()

    @pl.when((step < n_seqs * DENSE_EVERY) & (lax.rem(step, DENSE_EVERY) == 0))
    def _():
        y_ref[0] = lax.dot_general(h_ref[0], wo_ref[...], (((1,), (0,)), ((), ())), preferred_element_type=F32).astype(BF16)
        total = lax.dot_general(dg_ref[0], wg_ref[...], (((1,), (1,)), ((), ())), preferred_element_type=F32)
        for grad_ref, w_ref in ((dl_ref, wb_ref), (dq_ref, wq_ref), (dk_ref, wk_ref), (dv_ref, wv_ref)):
            total = total + lax.dot_general(grad_ref[0], w_ref[...], (((1,), (1,)), ((), ())), preferred_element_type=F32)
        dx_ref[0] = total.astype(BF16)

    @pl.when(step < n_chunks)
    def _():
        own[rows(step)] = own[rows(step)] + pair[rows(step)]

    @pl.when(is_mid & (step >= LAG_JOIN) & (step < n_chunks + LAG_JOIN))
    def _():
        idx = step - LAG_JOIN
        outer_copy(pair, idx).wait_recv()
        own[rows(idx)] = own[rows(idx)] + outer[rows(idx)]

    @pl.when(is_mid & (step >= LAG_TOTAL) & (step < n_chunks + LAG_TOTAL))
    def _():
        idx = step - LAG_TOTAL
        inner_copy(idx).wait_recv()
        pair[rows(idx)] = own[rows(idx)] + inner[rows(idx)]

    @pl.when(is_end & (step >= LAG_END) & (step < n_chunks + LAG_END))
    def _():
        outer_copy(own, step - LAG_END).wait_recv()

    for idx in range(len(parts)):
        final = idx * group_len + parts[idx].shape[0] // 2 // CHUNK - 1

        @pl.when(is_end & (step == final + LAG_END))
        def _():
            store_copy(outer, idx).start()
            give_copy(outer, idx).start()

    @pl.when(step == last_step)
    def _():
        for idx in range(len(parts)):
            pair_copy(idx).wait_send()
            store_copy(outer, idx).wait()
            give_copy(outer, idx).wait()

        def drain_outer(idx, carry):
            outer_copy(own, idx).wait_send()
            return carry

        lax.fori_loop(0, n_chunks, drain_outer, 0)

        @pl.when(is_mid)
        def _():
            def drain_inner(idx, carry):
                inner_copy(idx).wait_send()
                return carry

            lax.fori_loop(0, n_chunks, drain_inner, 0)


def run_tail(parts, acts, weights):
    n_seqs, seq_dev, model_dim = acts[0].shape
    n_rows = sum(part.shape[0] for part in parts) // 2
    n_chunks = n_rows // CHUNK
    n_parts = len(parts)
    any_spec = pl.BlockSpec(memory_space=pl.ANY)

    def row_block(arr):
        return pl.BlockSpec((1,) + tuple(arr.shape[1:]), lambda step: (jnp.minimum(step // DENSE_EVERY, n_seqs - 1), 0, 0))

    outs = [jax.ShapeDtypeStruct(part.shape, F32) for part in parts] + [jax.ShapeDtypeStruct(acts[0].shape, BF16)] * 2
    buf = pltpu.VMEM((n_rows, model_dim), F32)
    part_sems = pltpu.SemaphoreType.DMA((n_parts,))
    chunk_sems = pltpu.SemaphoreType.DMA((n_chunks,))
    return pl.pallas_call(
        functools.partial(tail_kernel, n_seqs),
        grid=(n_chunks + LAG_END + 1,),
        out_shape=outs,
        in_specs=[any_spec] * n_parts + [row_block(arr) for arr in acts] + [pl.BlockSpec(memory_space=pltpu.VMEM) for _ in weights],
        out_specs=[any_spec] * n_parts + [row_block(acts[0])] * 2,
        scratch_shapes=[buf] * 4 + [part_sems] * 3 + [chunk_sems] * 4 + [part_sems] * 3,
        compiler_params=pltpu.CompilerParams(collective_id=2, has_side_effects=True, vmem_limit_bytes=62 * 1024 * 1024, dimension_semantics=('arbitrary',)),
        cost_estimate=pl.CostEstimate(flops=250_000_000_000, bytes_accessed=120_000_000, transcendentals=0),
        name='sum_and_project',
    )(*parts, *acts, *weights)


def solution(mesh):
    groups = mesh.shape['sp']
    to_next = [(source, source + 1) for source in range(groups - 1)]
    seq_spec = P('dp', 'sp', None)
    full_mat = P(None, None)
    part_mat = P('dp', None)

    def local_step(x_in, dy_out, w_query, w_key, w_value, w_beta, conv_query, conv_key, conv_value, w_gate, norm_weight, w_out):
        seq_dev = x_in.shape[1]
        projs = [project(x_in, weight).astype(BF16) for weight in (w_query, w_key, w_value)]
        tails = lax.ppermute(jnp.concatenate([proj[:, seq_dev - PAD:] for proj in projs], axis=-1), 'sp', to_next)
        taps = jnp.stack([conv_query, conv_key, conv_value]).astype(F32)
        logits = project(x_in, w_beta).astype(BF16)
        gate_pre = project(x_in, w_gate).astype(BF16)
        d_hidden = back_project(dy_out, w_out).astype(BF16)
        norm_f = norm_weight.astype(F32).reshape(1, HEAD_DIM)
        hidden, d_gate, d_attn, q_act, k_act, t_mat, s_mat, r_mat, d_mat, dnorm = run_forward(groups, projs, tails, taps, logits, gate_pre, d_hidden, norm_f)
        dp_q, dp_k, dp_v, d_logit, dtaps = run_backward(groups, projs, tails, taps, logits, d_attn, q_act, k_act, t_mat, s_mat, r_mat, d_mat)
        model_dim = x_in.shape[2]
        small = jnp.concatenate([
            jnp.einsum('bte,btd->ed', d_logit, x_in, preferred_element_type=F32),
            jnp.sum(dtaps, axis=2).reshape(3 * CONV_TAPS, model_dim),
            jnp.pad(jnp.sum(dnorm, axis=0, keepdims=True), ((0, 0), (0, model_dim - HEAD_DIM)))])
        n_heads = w_beta.shape[1]
        small = jnp.pad(small, ((0, 2 * CHUNK - small.shape[0]), (0, 0)))
        grads = (weight_grad(x_in, d_gate), weight_grad(hidden, dy_out), weight_grad(x_in, dp_q), weight_grad(x_in, dp_k), weight_grad(x_in, dp_v), small)
        dw_gate, dw_out, dw_q, dw_k, dw_v, small, y_out, dx_in = run_tail(
            grads, (hidden, d_gate, dp_q, dp_k, dp_v, d_logit), (w_out, w_gate, w_query, w_key, w_value, w_beta))
        dtaps = small[n_heads:n_heads + 3 * CONV_TAPS].reshape(3, CONV_TAPS, model_dim)
        dnorm = small[n_heads + 3 * CONV_TAPS, :HEAD_DIM]
        return (y_out, dx_in, dw_q, dw_k, dw_v, small[:n_heads].T, dtaps[0], dtaps[1], dtaps[2], dw_gate, dnorm, dw_out)

    in_specs = (seq_spec, seq_spec) + (full_mat,) * 8 + (P(None), full_mat)
    out_specs = (seq_spec, seq_spec) + (part_mat,) * 8 + (P('dp'), part_mat)
    return jax.shard_map(local_step, mesh=mesh, in_specs=in_specs, out_specs=out_specs, check_vma=False)
```
